32 devices in a mesh: cp: 16 (over z, x, core), tp: 2 (over y).
Axes of the slice: x: 2, y: 2, z: 4, core: 2. Of those that a mesh axis runs over, the one named last changes fastest.
Arguments:
- query: bfloat16 [1024, 16384], P(('cp', 'tp')), may hold values from -6 to 6
- fresh_key_rows: bfloat16 [1024, 1024], P(('cp', 'tp')), may hold values from -6 to 6
- fresh_value_rows: bfloat16 [1024, 1024], P(('cp', 'tp')), may hold values from -6 to 6
- cached_key_rows: bfloat16 [8192, 1024], P('cp', 'tp'), may hold values from -6 to 6
- cached_value_rows: bfloat16 [8192, 1024], P('cp', 'tp'), may hold values from -6 to 6
- prefix_len: int32 [1], replicated, may hold values from 4096 to 8192
- stripe_owner: int32 [16], replicated, may hold values from 0 to 15, each once
Outputs:
- attended: bfloat16 [1024, 16384], P('cp', 'tp')
The draws below stay inside these ranges and needn't reach their ends.
Inputs may be any that keep to these rules, and one draw needn't show every extreme that they name: `stripe_owner`: a permutation of 0 to 15.
All inputs are finite; a program needn't handle non-finite values.
Results may differ from the reference program's by a relative error of at most 0.0075.
Values may be sent and summed in bfloat16 or wider, within the bound.
A program may use at most 64 MiB of HBM per device.

```python
import math
import jax
import jax.numpy as jnp
from jax import lax

QUERY_HEADS = 128
KEY_VALUE_HEADS = 8
HEAD_SIZE = 128
TOK_DEV = 64
NEW_TOKENS = 1024
CACHE_SLOTS = 8192
N_CP = 16


def draw_query(key, part):
    base_offset = jnp.clip(jax.random.normal(jax.random.fold_in(key, 11), (NEW_TOKENS, QUERY_HEADS * HEAD_SIZE), jnp.float32), -6.0, 6.0)
    return base_offset.astype(jnp.bfloat16)


def draw_cached_key_rows(key, part):
    base_offset = jnp.clip(jax.random.normal(jax.random.fold_in(key, 12), (CACHE_SLOTS, KEY_VALUE_HEADS * HEAD_SIZE), jnp.float32), -6.0, 6.0)
    return base_offset.astype(jnp.bfloat16)


def level_of(rng, extent, shards, low, largest):
    def one(dim, parts):
        heights = jax.random.uniform(jax.random.fold_in(jax.random.fold_in(rng, 6), dim), (parts,), jnp.float32, low / len(shards), largest / len(shards))
        return jnp.repeat(jnp.exp(heights), extent[dim] // parts).reshape((-1,) + (1,) * (len(extent) - dim - 1))

    gain = one(*shards[0])
    for cut in shards[1:]:
        gain = gain * one(*cut)
    return gain


def bell_draw(key, shape, width, most, shards=(), kind=jnp.bfloat16):
    values = jax.random.normal(key, shape, jnp.float32) * width
    if len(shards) > 0:
        values = level_of(key, shape, shards, -0.22, 0.18) * values
    return jnp.clip(values, min=-most, max=most).astype(kind)


def setup_inputs(seed: int = 0) -> dict:
    seeds = jax.random.split(jax.random.key(seed), 8)
    query = draw_query(jax.random.fold_in(seeds[7], 71), 0)
    fresh_key_rows = bell_draw(seeds[1], (NEW_TOKENS, KEY_VALUE_HEADS * HEAD_SIZE), 1.0, 6.0, ((0, 32),))
    fresh_value_rows = bell_draw(seeds[2], (NEW_TOKENS, KEY_VALUE_HEADS * HEAD_SIZE), 1.0, 6.0, ((0, 32),))
    cached_key_rows = draw_cached_key_rows(jax.random.fold_in(seeds[7], 71), 0)
    cached_value_rows = bell_draw(seeds[4], (CACHE_SLOTS, KEY_VALUE_HEADS * HEAD_SIZE), 1.0, 6.0, ((0, 16), (1, 2)))
    prefix_len = jax.random.randint(seeds[5], (1,), CACHE_SLOTS // 2, CACHE_SLOTS + 1).astype(jnp.int32)
    stripe_owner = jax.random.permutation(seeds[6], N_CP).astype(jnp.int32)
    return {"query": query, "fresh_key_rows": fresh_key_rows, "fresh_value_rows": fresh_value_rows, "cached_key_rows": cached_key_rows, "cached_value_rows": cached_value_rows, "prefix_len": prefix_len, "stripe_owner": stripe_owner}


NEG = -1.0e30


def reference(query, fresh_key_rows, fresh_value_rows, cached_key_rows, cached_value_rows, prefix_len, stripe_owner):
    group_size = QUERY_HEADS // KEY_VALUE_HEADS
    scale = HEAD_SIZE ** -0.5
    plen = prefix_len[0]
    block_number = math.gcd(NEW_TOKENS, 256)
    block_count = NEW_TOKENS // block_number
    cache_live = jnp.arange(CACHE_SLOTS, dtype=jnp.int32) < plen
    new_index = jnp.arange(NEW_TOKENS, dtype=jnp.int32)
    combined_keys = jnp.concatenate([cached_key_rows.reshape(CACHE_SLOTS, KEY_VALUE_HEADS, HEAD_SIZE), fresh_key_rows.reshape(NEW_TOKENS, KEY_VALUE_HEADS, HEAD_SIZE)], axis=0).transpose(1, 0, 2)
    combined_values = jnp.concatenate([cached_value_rows.reshape(CACHE_SLOTS, KEY_VALUE_HEADS, HEAD_SIZE), fresh_value_rows.reshape(NEW_TOKENS, KEY_VALUE_HEADS, HEAD_SIZE)], axis=0).transpose(1, 0, 2)
    query_head_rows = query.reshape(block_count, block_number, KEY_VALUE_HEADS, group_size, HEAD_SIZE).transpose(2, 0, 1, 3, 4)

    def per_head(inputs):
        queries, keys, values = inputs
        keys32 = keys.astype(jnp.float32)
        values32 = values.astype(jnp.float32)

        def per_block(pair):
            rows, number = pair
            query_index = number * block_number + jnp.arange(block_number, dtype=jnp.int32)
            scores = jnp.einsum("qgd,kd->gqk", rows.astype(jnp.float32), keys32) * scale
            visible = jnp.concatenate([jnp.broadcast_to(cache_live[None, :], (block_number, CACHE_SLOTS)), new_index[None, :] <= query_index[:, None]], axis=1)
            peak = jnp.max(jnp.where(visible, scores, NEG), axis=-1, keepdims=True)
            weights = jnp.where(visible, jnp.exp(scores - peak), 0.0)
            total = jnp.sum(weights, axis=-1, keepdims=True)
            rounded = lax.optimization_barrier(weights.astype(jnp.bfloat16)).astype(jnp.float32)
            result = jnp.einsum("gqk,kd->gqd", rounded, values32) / total
            return result.astype(jnp.bfloat16)

        return lax.map(per_block, (queries, jnp.arange(block_count, dtype=jnp.int32)))

    outputs = lax.map(per_head, (query_head_rows, combined_keys, combined_values))
    natural = outputs.transpose(1, 3, 0, 2, 4).reshape(NEW_TOKENS, QUERY_HEADS * HEAD_SIZE)
    inverse = jnp.argsort(stripe_owner).astype(jnp.int32)
    stripe = TOK_DEV // N_CP
    arranged = natural.reshape(N_CP, N_CP, stripe, QUERY_HEADS * HEAD_SIZE)[:, inverse]
    return arranged.transpose(1, 0, 2, 3).reshape(NEW_TOKENS, QUERY_HEADS * HEAD_SIZE)
```

```python
import functools
import math

import jax
import jax.numpy as jnp
from jax import lax
from jax.experimental import pallas as pl
from jax.experimental.pallas import tpu as pltpu
from jax.sharding import PartitionSpec as P

HEAD_SIZE = 128
NEG = -1e30
EXPONENT = HEAD_SIZE ** (-0.5) * math.log2(math.e)


def attend_kernel(dims, plen_ref, q_ref, nat_ref, fresh_k, fresh_v, cache_k, cache_v, out_ref,
                  k2, vt, q2, s0, s1, m_ref, l_ref, acc_ref):
    per_step, chunk = dims
    rows = q_ref.shape[0]
    wide = rows * per_step
    plen = plen_ref[0]
    fresh, slots = fresh_k.shape[0], cache_k.shape[0]
    dn = (((1,), (1,)), ((), ()))

    @pl.when(pl.program_id(0) == 0)
    def _():
        eye = (lax.broadcasted_iota(jnp.int32, (HEAD_SIZE, HEAD_SIZE), 0)
               == lax.broadcasted_iota(jnp.int32, (HEAD_SIZE, HEAD_SIZE), 1)).astype(jnp.bfloat16)
        step = min(512, fresh)

        def prepare(source_k, source_v, base, count):
            def body(b, _):
                at = pl.multiple_of(b * step, step)
                to = pl.multiple_of(base + b * step, step)
                k = source_k[pl.ds(at, step), :]
                k2[pl.ds(to, step), :HEAD_SIZE] = k
                k2[pl.ds(to, step), HEAD_SIZE:] = k
                v = source_v[pl.ds(at, step), :]
                vt[:, pl.ds(to, step)] = lax.dot_general(
                    eye, v, dn, preferred_element_type=jnp.float32).astype(jnp.bfloat16)
                return 0
            lax.fori_loop(0, count // step, body, 0)
        prepare(fresh_k, fresh_v, 0, fresh)
        prepare(cache_k, cache_v, fresh, slots)

    for g in range(per_step):
        x = q_ref[:, g * HEAD_SIZE:(g + 1) * HEAD_SIZE].astype(jnp.float32) * EXPONENT
        x = x.T
        hi = x.astype(jnp.bfloat16)
        q2[:HEAD_SIZE, g * rows:(g + 1) * rows] = hi
        q2[HEAD_SIZE:, g * rows:(g + 1) * rows] = (x - hi.astype(jnp.float32)).astype(jnp.bfloat16)

    def score(at, s):
        s[...] = jnp.dot(k2[pl.ds(at, chunk), :], q2[...], preferred_element_type=jnp.float32)

    def soften(at, s_ref, mask, first):
        s = s_ref[...]
        if mask is not None:
            s = jnp.where(mask, s, NEG)
        top = jnp.max(s, axis=0, keepdims=True)
        m_new = top if first else jnp.maximum(m_ref[...], top)
        p = jnp.exp2(s - m_new)
        total = jnp.sum(p, axis=0, keepdims=True)
        o = jnp.dot(vt[:, pl.ds(at, chunk)], p.astype(jnp.bfloat16), preferred_element_type=jnp.float32)
        if first:
            l_ref[...] = total
            acc_ref[...] = o
        else:
            f = jnp.exp2(m_ref[...] - m_new)
            l_ref[...] = f * l_ref[...] + total
            acc_ref[...] = f * acc_ref[...] + o
        m_ref[...] = m_new

    bufs = (s0, s1)
    number = fresh // chunk
    assert number % 2 == 0
    nat = nat_ref[...]
    index = lax.broadcasted_iota(jnp.int32, (chunk, wide), 0)
    score(0, s0)
    for c in range(number):
        score((c + 1) * chunk, bufs[(c + 1) % 2])
        soften(c * chunk, bufs[c % 2], index + c * chunk <= nat, c == 0)

    pairs = (plen + 2 * chunk - 1) // (2 * chunk)

    def body(j, _):
        at = pl.multiple_of(fresh + 2 * j * chunk, chunk)
        score(pl.multiple_of(at + chunk, chunk), s1)
        soften(at, s0, None, False)
        score(pl.multiple_of(at + 2 * chunk, chunk), s0)
        soften(pl.multiple_of(at + chunk, chunk), s1, None, False)
        return 0
    lax.fori_loop(0, pairs - 1, body, 0)
    slot = 2 * (pairs - 1) * chunk
    at = pl.multiple_of(fresh + slot, chunk)
    score(pl.multiple_of(at + chunk, chunk), s1)
    soften(at, s0, index + slot < plen, False)
    soften(pl.multiple_of(at + chunk, chunk), s1, index + (slot + chunk) < plen, False)

    done = acc_ref[...] / l_ref[...]
    for g in range(per_step):
        out_ref[:, g * HEAD_SIZE:(g + 1) * HEAD_SIZE] = done[:, g * rows:(g + 1) * rows].T.astype(out_ref.dtype)


def attend(q, nat, fresh_k, fresh_v, cache_k, cache_v, prefix_len, chunk=512):
    rows, columns = q.shape
    per_step = nat.shape[1] // rows
    width = per_step * HEAD_SIZE
    wide = per_step * rows
    fresh, slots = fresh_k.shape[0], cache_k.shape[0]
    whole = lambda i, *_: (0, 0)
    keys = fresh + slots
    return pl.pallas_call(
        functools.partial(attend_kernel, (per_step, chunk)),
        out_shape=jax.ShapeDtypeStruct((rows, columns), jnp.bfloat16),
        grid_spec=pltpu.PrefetchScalarGridSpec(
            num_scalar_prefetch=1,
            grid=(columns // width,),
            in_specs=[
                pl.BlockSpec((rows, width), lambda i, *_: (0, i)),
                pl.BlockSpec((1, wide), whole),
                pl.BlockSpec((fresh, HEAD_SIZE), whole),
                pl.BlockSpec((fresh, HEAD_SIZE), whole),
                pl.BlockSpec((slots, HEAD_SIZE), whole),
                pl.BlockSpec((slots, HEAD_SIZE), whole),
            ],
            out_specs=pl.BlockSpec((rows, width), lambda i, *_: (0, i)),
            scratch_shapes=[
                pltpu.VMEM((keys, 2 * HEAD_SIZE), jnp.bfloat16),
                pltpu.VMEM((HEAD_SIZE, keys), jnp.bfloat16),
                pltpu.VMEM((2 * HEAD_SIZE, wide), jnp.bfloat16),
                pltpu.VMEM((chunk, wide), jnp.float32),
                pltpu.VMEM((chunk, wide), jnp.float32),
                pltpu.VMEM((1, wide), jnp.float32),
                pltpu.VMEM((1, wide), jnp.float32),
                pltpu.VMEM((HEAD_SIZE, wide), jnp.float32),
            ],
        ),
        compiler_params=pltpu.CompilerParams(vmem_limit_bytes=56 * 1024 * 1024),
        cost_estimate=pl.CostEstimate(flops=4*rows*columns*keys, bytes_accessed=4 * keys*HEAD_SIZE, transcendentals=0),
    )(prefix_len, q, nat, fresh_k, fresh_v, cache_k, cache_v)


def remote(source, target, send, receive, device):
    return pltpu.make_async_remote_copy(
        src_ref=source,
        dst_ref=target,
        send_sem=send,
        recv_sem=receive,
        device_id=device,
        device_id_type=pl.DeviceIdType.MESH,
    )


def greet(devices):
    barrier = pltpu.get_barrier_semaphore()
    for device in devices:
        pl.semaphore_signal(
            barrier, inc=1, device_id=device, device_id_type=pl.DeviceIdType.MESH
        )
    pl.semaphore_wait(barrier, len(devices))


def fused_kernel(
    sizes,
    plen_ref,
    nat_ref,
    pick_ref,
    query,
    fresh_k,
    fresh_v,
    cache_k,
    cache_v,
    out,
    k2,
    v_land,
    vt,
    q_land,
    o_buf,
    q2,
    s0,
    s1,
    m_ref,
    l_ref,
    acc_ref,
    fresh_send,
    fresh_recv,
    z_send,
    z_recv,
    q_send,
    q_recv,
    o_send,
    o_recv,
    *rank_sems,
):
    heads, ranks, tps, per_step, chunk = sizes
    parts = heads * ranks
    me, tp = lax.axis_index("cp"), lax.axis_index("tp")
    row, rank = me // ranks, me % ranks
    few = fresh_k.shape[0]
    block = cache_k.shape[0]
    fresh = parts * tps * few
    keys = k2.shape[0]
    slots = keys - fresh
    steps, rows, width = q_land.shape
    own_columns = steps * width
    wide = per_step * rows
    share = rows // parts
    dn = (((1,), (1,)), ((), ()))

    bits = []
    bit = ranks // 2
    while bit:
        bits.append(bit)
        bit //= 2
    partners = [rank + bit - 2 * bit * ((rank // bit) % 2) for bit in bits]
    line = [{"cp": row * ranks + partner} for partner in partners]

    def at_column(s, t):
        return {"cp": (row + s) % heads * ranks + rank, "tp": (tp + t) % tps}

    greet(
        [{"cp": (me + d) % parts} for d in range(1, parts)]
        + [at_column(s, t) for s in range(heads) for t in range(1, tps)]
    )

    def span(ref, start, size, step):
        return ref.at[pl.ds(pl.multiple_of(start, step), size), pl.ds(0, HEAD_SIZE)]

    def cut(ref, head):
        return ref.at[:, pl.ds(pl.multiple_of(head * HEAD_SIZE, HEAD_SIZE), HEAD_SIZE)]

    def place(a, index):
        target = k2 if a % 2 == 0 else v_land
        if a < 2:
            return span(target, fresh + index * block, block, block)
        return span(target, index * (tps * few), tps * few, tps * few)

    far = sorted(range(1, heads), key=lambda s: abs(2 * s - heads))
    shifts = [0] + far
    started = []

    def go(copy):
        copy.start()
        started.append(copy)
        return copy

    arrived = {}
    for s in shifts:
        for a, source in enumerate((cache_k, cache_v)):
            piece = cut(source, (row + s) % heads)
            if s == 0:
                copy = pltpu.make_async_copy(piece, place(a, me), z_recv.at[a, s])
                copy.start()
                arrived[a, s] = [copy.wait]
            else:
                copy = go(
                    remote(piece, place(a, me), z_send.at[a, s], z_recv.at[a, s], at_column(s, 0))
                )
                arrived[a, s] = [copy.wait_recv]
        for a, source in enumerate((fresh_k, fresh_v)):
            waits = []
            for t in range(tps):
                to = at_column(s, t)
                piece = cut(source, to["tp"] * heads + (row + s) % heads)
                target = span((k2, v_land)[a], me * (tps * few) + tp * few, few, few)
                if s == 0 and t == 0:
                    copy = pltpu.make_async_copy(piece, target, fresh_recv.at[a, s, t])
                    copy.start()
                    waits.append(copy.wait)
                else:
                    copy = go(
                        remote(
                            piece, target, fresh_send.at[a, s, t], fresh_recv.at[a, s, t], to
                        )
                    )
                    waits.append(copy.wait_recv)
            arrived[2 + a, s] = waits

    def query_copy(g, s, t, local):
        to = at_column(s, t)
        start = (to["tp"] * heads + (row + s) % heads) * own_columns + g * width
        source = query.at[:, pl.ds(pl.multiple_of(start, width), width)]
        target = q_land.at[g, pl.ds(pl.multiple_of((row * tps + tp) * few, few), few), :]
        if local:
            return pltpu.make_async_copy(source, target, q_recv.at[g, 0])
        return remote(source, target, q_send.at[g, s * tps + t], q_recv.at[g, s * tps + t], to)

    routes = [(s, t) for s in shifts for t in range(tps)]

    def send_query(g, _):
        for s, t in routes:
            query_copy(g, s, t, s == 0 and t == 0).start()
        return 0

    lax.fori_loop(0, steps, send_query, 0)

    order = (2, 3, 0, 1)
    held = [((a, s), a, s, rank) for s in shifts for a in order]
    for level, partner in enumerate(partners):
        send, receive = rank_sems[2 * level], rank_sems[2 * level + 1]
        other = []
        for number, (key, a, s, owner) in enumerate(held):
            for wait in arrived.pop(key, ()):
                wait()
            index = (row + heads - s) % heads * ranks + owner
            copy = go(
                remote(
                    place(a, index), place(a, index), send.at[number], receive.at[number], line[level]
                )
            )
            bit = bits[level]
            name = (a, s, level + 1, number)
            arrived[name] = [copy.wait_recv]
            other.append((name, a, s, owner + bit - 2 * bit * ((owner // bit) % 2)))
        held = held + other
    for waits in arrived.values():
        for wait in waits:
            wait()

    eye = (
        lax.broadcasted_iota(jnp.int32, (HEAD_SIZE, HEAD_SIZE), 0)
        == lax.broadcasted_iota(jnp.int32, (HEAD_SIZE, HEAD_SIZE), 1)
    ).astype(jnp.bfloat16)

    def prepare(b, _):
        at = pl.multiple_of(b * chunk, chunk)
        k2[pl.ds(at, chunk), HEAD_SIZE:] = k2[pl.ds(at, chunk), :HEAD_SIZE]
        vt[:, pl.ds(at, chunk)] = lax.dot_general(
            eye, v_land[pl.ds(at, chunk), :], dn, preferred_element_type=jnp.float32
        ).astype(jnp.bfloat16)
        return 0

    lax.fori_loop(0, keys // chunk, prepare, 0)

    def score(at, s):
        s[...] = jnp.dot(k2[pl.ds(at, chunk), :], q2[...], preferred_element_type=jnp.float32)

    def soften(at, s_ref, mask, first):
        s = s_ref[...]
        if mask is not None:
            s = jnp.where(mask, s, NEG)
        top = jnp.max(s, axis=0, keepdims=True)
        m_new = top if first else jnp.maximum(m_ref[...], top)
        p = jnp.exp2(s - m_new)
        total = jnp.sum(p, axis=0, keepdims=True)
        o = jnp.dot(
            vt[:, pl.ds(at, chunk)], p.astype(jnp.bfloat16), preferred_element_type=jnp.float32
        )
        if first:
            l_ref[...] = total
            acc_ref[...] = o
        else:
            f = jnp.exp2(m_ref[...] - m_new)
            l_ref[...] = f * l_ref[...] + total
            acc_ref[...] = f * acc_ref[...] + o
        m_ref[...] = m_new

    def output_copy(g, d):
        to = (me + d) % parts
        columns = pl.ds(pl.multiple_of(g * width, width), width)
        source = o_buf.at[pl.ds(pl.multiple_of(to * share, share), share), columns]
        target = out.at[
            pl.ds(pl.multiple_of(rank * share, share), share),
            pl.ds(pl.multiple_of(row * own_columns + g * width, width), width),
        ]
        if d == 0:
            return pltpu.make_async_copy(source, target, o_recv.at[g, 0])
        return remote(source, target, o_send.at[g, d], o_recv.at[g, d], {"cp": to})

    def send_output(g):
        for d in range(parts):
            output_copy(g, d).start()

    bufs = (s0, s1)
    number = fresh // chunk
    index = lax.broadcasted_iota(jnp.int32, (chunk, wide), 0)
    pairs = slots // (2 * chunk)
    sure = pairs // 2

    def step(g, _):
        for s, t in routes:
            if s == 0 and t == 0:
                query_copy(g, s, t, True).wait()
            else:
                query_copy(g, s, t, False).wait_recv()
        pick = pick_ref[...]
        for h in range(per_step):
            x = jnp.dot(
                pick,
                q_land[g, :, h * HEAD_SIZE : (h + 1) * HEAD_SIZE],
                preferred_element_type=jnp.float32,
            )
            x = x.T * EXPONENT
            hi = x.astype(jnp.bfloat16)
            q2[:HEAD_SIZE, h * rows : (h + 1) * rows] = hi
            q2[HEAD_SIZE:, h * rows : (h + 1) * rows] = (x - hi.astype(jnp.float32)).astype(
                jnp.bfloat16
            )

        @pl.when(g > 0)
        def _():
            send_output(g - 1)

        nat = nat_ref[...]
        score(0, s0)
        for c in range(number):
            score((c + 1) * chunk, bufs[(c + 1) % 2])
            soften(c * chunk, bufs[c % 2], index + c * chunk <= nat, c == 0)

        def pair(masked, last, j):
            slot = 2 * j * chunk
            at = pl.multiple_of(fresh + slot, chunk)
            score(pl.multiple_of(at + chunk, chunk), s1)
            soften(at, s0, index + slot < plen_ref[...] if masked else None, False)
            if not last:
                score(pl.multiple_of(at + 2 * chunk, chunk), s0)
            soften(
                pl.multiple_of(at + chunk, chunk),
                s1,
                index + (slot + chunk) < plen_ref[...] if masked else None,
                False,
            )

        def plain(j, _):
            pair(False, False, j)
            return 0

        def masked(j, _):
            pair(True, False, j)
            return 0

        lax.fori_loop(0, sure, plain, 0)
        lax.fori_loop(sure, pairs - 1, masked, 0)
        pair(True, True, pairs - 1)

        done = acc_ref[...] / l_ref[...]
        for h in range(per_step):
            columns = pl.ds(pl.multiple_of(g * width + h * HEAD_SIZE, HEAD_SIZE), HEAD_SIZE)
            o_buf[:, columns] = done[:, h * rows : (h + 1) * rows].T.astype(o_buf.dtype)
        return 0

    lax.fori_loop(0, steps, step, 0)
    send_output(steps - 1)

    def finish(g, _):
        for s, t in routes:
            if s != 0 or t != 0:
                query_copy(g, s, t, False).wait_send()
        for d in range(parts):
            output_copy(g, d).wait()
        return 0

    for copy in started:
        copy.wait_send()
    lax.fori_loop(0, steps, finish, 0)


def fused(
    plen, nat, pick, query, fresh_k, fresh_v, cache_k, cache_v, heads, ranks, tps, per_step, chunk
):
    parts = heads * ranks
    few, block = fresh_k.shape[0], cache_k.shape[0]
    fresh = parts * tps * few
    keys = fresh + parts * block
    rows = heads * tps * few
    width = per_step * HEAD_SIZE
    wide = per_step * rows
    own_columns = query.shape[1] // (tps * heads)
    steps = own_columns // width
    rank_sems = []
    count = 4 * heads
    size = ranks
    while size > 1:
        rank_sems += [pltpu.SemaphoreType.DMA((count,))] * 2
        count *= 2
        size //= 2
    dma = pltpu.SemaphoreType.DMA
    b16, f32 = jnp.bfloat16, jnp.float32
    return pl.pallas_call(
        functools.partial(fused_kernel, (heads, ranks, tps, per_step, chunk)),
        out_shape=jax.ShapeDtypeStruct((tps * few, heads * own_columns), b16),
        in_specs=[pl.BlockSpec(memory_space=pltpu.VMEM)] * 3
        + [pl.BlockSpec(memory_space=pl.ANY)] * 5,
        out_specs=pl.BlockSpec(memory_space=pl.ANY),
        scratch_shapes=[
            pltpu.VMEM((keys, 2 * HEAD_SIZE), b16),
            pltpu.VMEM((keys, HEAD_SIZE), b16),
            pltpu.VMEM((HEAD_SIZE, keys), b16),
            pltpu.VMEM((steps, rows, width), b16),
            pltpu.VMEM((rows, own_columns), b16),
            pltpu.VMEM((2 * HEAD_SIZE, wide), b16),
            pltpu.VMEM((chunk, wide), f32),
            pltpu.VMEM((chunk, wide), f32),
            pltpu.VMEM((1, wide), f32),
            pltpu.VMEM((1, wide), f32),
            pltpu.VMEM((HEAD_SIZE, wide), f32),
            dma((2, heads, tps)),
            dma((2, heads, tps)),
            dma((2, heads)),
            dma((2, heads)),
            dma((steps, heads * tps)),
            dma((steps, heads * tps)),
            dma((steps, parts)),
            dma((steps, parts)),
        ]
        + rank_sems,
        compiler_params=pltpu.CompilerParams(
            collective_id=1, has_side_effects=True, vmem_limit_bytes=56 * 1024 * 1024
        ),
        cost_estimate=pl.CostEstimate(
            flops=4 * rows * own_columns * keys, bytes_accessed=100000000, transcendentals=0
        ),
    )(plen, nat, pick, query, fresh_k, fresh_v, cache_k, cache_v)


def exchanged(
    query, fresh_key_rows, fresh_value_rows, cached_key_rows, cached_value_rows, prefix_len, inverse
):
    parts, tps = lax.axis_size("cp"), lax.axis_size("tp")
    heads = cached_key_rows.shape[1] // HEAD_SIZE
    ranks = parts // heads
    rank = lax.axis_index("cp") % ranks
    few = fresh_key_rows.shape[0]
    many = tps * few
    stripe = many // parts
    rows = heads * many
    group = query.shape[1] // (tps * heads * HEAD_SIZE)
    per_step = max(1, min(group, 512 // rows))
    fresh = parts * many
    chunk = min(512, fresh // 2)
    z = jnp.arange(heads, dtype=jnp.int32)[None, :, None]
    i = jnp.arange(stripe, dtype=jnp.int32)[None, None, :]
    inside = inverse[:, None, None] * stripe + i
    local = (z * many + inside).reshape(rows)
    nat = ((z * ranks + rank) * many + inside).reshape(rows)
    nat = jnp.tile(nat[None, :], (1, per_step))
    pick = (local[:, None] == jnp.arange(rows, dtype=jnp.int32)[None, :]).astype(jnp.bfloat16)
    plen = jnp.broadcast_to(prefix_len[None, :], nat.shape)
    landed = fused(
        plen,
        nat,
        pick,
        query,
        fresh_key_rows,
        fresh_value_rows,
        cached_key_rows,
        cached_value_rows,
        heads,
        ranks,
        tps,
        per_step,
        chunk,
    )
    return (
        landed.reshape(ranks, heads, stripe, landed.shape[1])
        .transpose(1, 0, 2, 3)
        .reshape(landed.shape)
    )


def plain(
    query, fresh_key_rows, fresh_value_rows, cached_key_rows, cached_value_rows, prefix_len, inverse
):
    parts = lax.axis_size("cp")
    me = lax.axis_index("cp")
    heads = cached_key_rows.shape[1] // HEAD_SIZE
    ranks = parts // heads
    tps = lax.axis_size("tp")
    q_columns = query.shape[1] // tps // heads
    columns = [[h * ranks + r for h in range(heads)] for r in range(ranks)]
    lines = [[h * ranks + r for r in range(ranks)] for h in range(heads)]

    def split_heads(array, axis_name="cp"):
        if heads == 1:
            return array
        return lax.all_to_all(
            array, axis_name, split_axis=1, concat_axis=0, axis_index_groups=columns, tiled=True
        )

    def collect(array):
        block = array.shape[0]
        mine = split_heads(array)
        everything = lax.all_gather(mine, "cp", axis_index_groups=lines, tiled=True)
        return (
            everything.reshape(ranks, heads, block, HEAD_SIZE)
            .transpose(1, 0, 2, 3)
            .reshape(parts * block, HEAD_SIZE)
        )

    q_local = lax.all_to_all(query, "tp", split_axis=1, concat_axis=0, tiled=True)
    rows = q_local.shape[0]
    stripe = rows // parts
    by_rank = inverse.reshape(heads, ranks).T.reshape(-1)
    wanted = (by_rank[:, None] * stripe + jnp.arange(stripe, dtype=jnp.int32)[None, :]).reshape(-1)
    pick = (wanted[:, None] == jnp.arange(rows, dtype=jnp.int32)[None, :]).astype(jnp.bfloat16)
    q_sorted = jnp.dot(pick, q_local, preferred_element_type=jnp.float32).astype(jnp.bfloat16)
    q_out = (
        q_sorted.reshape(ranks, heads * stripe, heads, q_columns)
        .transpose(2, 0, 1, 3)
        .reshape(parts * heads * stripe, q_columns)
    )
    q_mine = lax.all_to_all(q_out, "cp", split_axis=0, concat_axis=0, tiled=True)
    own = [
        lax.all_to_all(array, "tp", split_axis=1, concat_axis=0, tiled=True)
        for array in (fresh_key_rows, fresh_value_rows)
    ]
    cache_k, cache_v, fresh_k, fresh_v = (
        collect(array) for array in (cached_key_rows, cached_value_rows, *own)
    )
    residues = jnp.take(by_rank.reshape(ranks, heads), me % ranks, axis=0)
    nat = (
        jnp.arange(parts, dtype=jnp.int32)[:, None, None] * rows
        + residues[None, :, None] * stripe
        + jnp.arange(stripe, dtype=jnp.int32)[None, None, :]
    ).reshape(1, -1)
    per_step = max(1, min(q_columns // HEAD_SIZE, 512 // nat.shape[1]))
    nat = jnp.tile(nat, (1, per_step))
    done = attend(q_mine, nat, fresh_k, fresh_v, cache_k, cache_v, prefix_len)
    done = (
        done.reshape(parts, heads, stripe, q_columns)
        .transpose(1, 0, 2, 3)
        .reshape(heads * rows, q_columns)
    )
    if heads == 1:
        return done
    split = done.reshape(heads, rows, q_columns)
    back = lax.all_to_all(
        split, "cp", split_axis=0, concat_axis=0, axis_index_groups=columns, tiled=True
    )
    return back.transpose(1, 0, 2).reshape(rows, heads * q_columns)


def shards(
    query,
    fresh_key_rows,
    fresh_value_rows,
    cached_key_rows,
    cached_value_rows,
    prefix_len,
    stripe_owner,
):
    parts = lax.axis_size("cp")
    heads = cached_key_rows.shape[1] // HEAD_SIZE
    ranks = parts // heads
    order = jnp.arange(parts, dtype=jnp.int32)
    inverse = jnp.sum(jnp.where(stripe_owner[None, :] == order[:, None], order[None, :], 0), axis=1)
    path = exchanged if heads > 1 and ranks & (ranks - 1) == 0 else plain
    return path(
        query,
        fresh_key_rows,
        fresh_value_rows,
        cached_key_rows,
        cached_value_rows,
        prefix_len,
        inverse,
    )


def solution(mesh):
    return jax.shard_map(
        shards,
        mesh=mesh,
        in_specs=(
            P(("cp", "tp"), None),
            P(("cp", "tp"), None),
            P(("cp", "tp"), None),
            P("cp", "tp"),
            P("cp", "tp"),
            P(),
            P(),
        ),
        out_specs=P("cp", "tp"),
        check_vma=False,
    )
```

```python
import functools
import math

import jax
import jax.numpy as jnp
from jax import lax
from jax.experimental import pallas as pl
from jax.experimental.pallas import tpu as pltpu
from jax.sharding import PartitionSpec as P

HEAD_SIZE = 128
NEG = -1e30
EXPONENT = HEAD_SIZE ** (-0.5) * math.log2(math.e)


def attend_kernel(dims, plen_ref, q_ref, nat_ref, fresh_k, fresh_v, cache_k, cache_v, out_ref,
                  k2, vt, q2, s0, s1, m_ref, l_ref, acc_ref):
    per_step, chunk = dims
    rows = q_ref.shape[0]
    wide = rows * per_step
    plen = plen_ref[0]
    fresh, slots = fresh_k.shape[0], cache_k.shape[0]
    dn = (((1,), (1,)), ((), ()))

    @pl.when(pl.program_id(0) == 0)
    def _():
        eye = (lax.broadcasted_iota(jnp.int32, (HEAD_SIZE, HEAD_SIZE), 0)
               == lax.broadcasted_iota(jnp.int32, (HEAD_SIZE, HEAD_SIZE), 1)).astype(jnp.bfloat16)
        step = min(512, fresh)

        def prepare(source_k, source_v, base, count):
            def body(b, _):
                at = pl.multiple_of(b * step, step)
                to = pl.multiple_of(base + b * step, step)
                k = source_k[pl.ds(at, step), :]
                k2[pl.ds(to, step), :HEAD_SIZE] = k
                k2[pl.ds(to, step), HEAD_SIZE:] = k
                v = source_v[pl.ds(at, step), :]
                vt[:, pl.ds(to, step)] = lax.dot_general(
                    eye, v, dn, preferred_element_type=jnp.float32).astype(jnp.bfloat16)
                return 0
            lax.fori_loop(0, count // step, body, 0)
        prepare(fresh_k, fresh_v, 0, fresh)
        prepare(cache_k, cache_v, fresh, slots)

    for g in range(per_step):
        x = q_ref[:, g * HEAD_SIZE:(g + 1) * HEAD_SIZE].astype(jnp.float32) * EXPONENT
        x = x.T
        hi = x.astype(jnp.bfloat16)
        q2[:HEAD_SIZE, g * rows:(g + 1) * rows] = hi
        q2[HEAD_SIZE:, g * rows:(g + 1) * rows] = (x - hi.astype(jnp.float32)).astype(jnp.bfloat16)

    def score(at, s):
        s[...] = jnp.dot(k2[pl.ds(at, chunk), :], q2[...], preferred_element_type=jnp.float32)

    def soften(at, s_ref, mask, first):
        s = s_ref[...]
        if mask is not None:
            s = jnp.where(mask, s, NEG)
        top = jnp.max(s, axis=0, keepdims=True)
        m_new = top if first else jnp.maximum(m_ref[...], top)
        p = jnp.exp2(s - m_new)
        total = jnp.sum(p, axis=0, keepdims=True)
        o = jnp.dot(vt[:, pl.ds(at, chunk)], p.astype(jnp.bfloat16), preferred_element_type=jnp.float32)
        if first:
            l_ref[...] = total
            acc_ref[...] = o
        else:
            f = jnp.exp2(m_ref[...] - m_new)
            l_ref[...] = f * l_ref[...] + total
            acc_ref[...] = f * acc_ref[...] + o
        m_ref[...] = m_new

    bufs = (s0, s1)
    number = fresh // chunk
    assert number % 2 == 0
    nat = nat_ref[...]
    index = lax.broadcasted_iota(jnp.int32, (chunk, wide), 0)
    score(0, s0)
    for c in range(number):
        score((c + 1) * chunk, bufs[(c + 1) % 2])
        soften(c * chunk, bufs[c % 2], index + c * chunk <= nat, c == 0)

    pairs = (plen + 2 * chunk - 1) // (2 * chunk)

    def body(j, _):
        at = pl.multiple_of(fresh + 2 * j * chunk, chunk)
        score(pl.multiple_of(at + chunk, chunk), s1)
        soften(at, s0, None, False)
        score(pl.multiple_of(at + 2 * chunk, chunk), s0)
        soften(pl.multiple_of(at + chunk, chunk), s1, None, False)
        return 0
    lax.fori_loop(0, pairs - 1, body, 0)
    slot = 2 * (pairs - 1) * chunk
    at = pl.multiple_of(fresh + slot, chunk)
    score(pl.multiple_of(at + chunk, chunk), s1)
    soften(at, s0, index + slot < plen, False)
    soften(pl.multiple_of(at + chunk, chunk), s1, index + (slot + chunk) < plen, False)

    done = acc_ref[...] / l_ref[...]
    for g in range(per_step):
        out_ref[:, g * HEAD_SIZE:(g + 1) * HEAD_SIZE] = done[:, g * rows:(g + 1) * rows].T.astype(out_ref.dtype)


def attend(q, nat, fresh_k, fresh_v, cache_k, cache_v, prefix_len, chunk=512):
    rows, columns = q.shape
    per_step = nat.shape[1] // rows
    width = per_step * HEAD_SIZE
    wide = per_step * rows
    fresh, slots = fresh_k.shape[0], cache_k.shape[0]
    whole = lambda i, *_: (0, 0)
    keys = fresh + slots
    return pl.pallas_call(
        functools.partial(attend_kernel, (per_step, chunk)),
        out_shape=jax.ShapeDtypeStruct((rows, columns), jnp.bfloat16),
        grid_spec=pltpu.PrefetchScalarGridSpec(
            num_scalar_prefetch=1,
            grid=(columns // width,),
            in_specs=[
                pl.BlockSpec((rows, width), lambda i, *_: (0, i)),
                pl.BlockSpec((1, wide), whole),
                pl.BlockSpec((fresh, HEAD_SIZE), whole),
                pl.BlockSpec((fresh, HEAD_SIZE), whole),
                pl.BlockSpec((slots, HEAD_SIZE), whole),
                pl.BlockSpec((slots, HEAD_SIZE), whole),
            ],
            out_specs=pl.BlockSpec((rows, width), lambda i, *_: (0, i)),
            scratch_shapes=[
                pltpu.VMEM((keys, 2 * HEAD_SIZE), jnp.bfloat16),
                pltpu.VMEM((HEAD_SIZE, keys), jnp.bfloat16),
                pltpu.VMEM((2 * HEAD_SIZE, wide), jnp.bfloat16),
                pltpu.VMEM((chunk, wide), jnp.float32),
                pltpu.VMEM((chunk, wide), jnp.float32),
                pltpu.VMEM((1, wide), jnp.float32),
                pltpu.VMEM((1, wide), jnp.float32),
                pltpu.VMEM((HEAD_SIZE, wide), jnp.float32),
            ],
        ),
        compiler_params=pltpu.CompilerParams(vmem_limit_bytes=56 * 1024 * 1024),
        cost_estimate=pl.CostEstimate(flops=4*rows*columns*keys, bytes_accessed=4 * keys*HEAD_SIZE, transcendentals=0),
    )(prefix_len, q, nat, fresh_k, fresh_v, cache_k, cache_v)


def remote(source, target, send, receive, device):
    return pltpu.make_async_remote_copy(
        src_ref=source,
        dst_ref=target,
        send_sem=send,
        recv_sem=receive,
        device_id=device,
        device_id_type=pl.DeviceIdType.MESH,
    )


def greet(devices):
    barrier = pltpu.get_barrier_semaphore()
    for device in devices:
        pl.semaphore_signal(
            barrier, inc=1, device_id=device, device_id_type=pl.DeviceIdType.MESH
        )
    pl.semaphore_wait(barrier, len(devices))


def fused_kernel(
    sizes,
    plen_ref,
    owner_ref,
    query,
    fresh_k,
    fresh_v,
    cache_k,
    cache_v,
    out,
    k2,
    v_land,
    vt,
    q_land,
    o_buf,
    q2,
    pick_ref,
    s0,
    s1,
    t0,
    t1,
    m_ref,
    l_ref,
    acc_ref,
    fresh_send,
    fresh_recv,
    z_send,
    z_recv,
    q_send,
    q_recv,
    o_send,
    o_recv,
    twin_sem,
    *rank_sems,
):
    heads, ranks, tps, per_step, chunk = sizes
    parts = heads * ranks
    me, tp = lax.axis_index("cp"), lax.axis_index("tp")
    row, rank = me // ranks, me % ranks
    few = fresh_k.shape[0]
    block = cache_k.shape[0]
    fresh = parts * tps * few
    keys = k2.shape[0]
    slots = keys - fresh
    steps, rows, width = q_land.shape
    own_columns = steps * width
    wide = per_step * rows
    share = rows // parts
    dn = (((1,), (1,)), ((), ()))

    bits = []
    bit = ranks // 2
    while bit:
        bits.append(bit)
        bit //= 2
    partners = [rank + bit - 2 * bit * ((rank // bit) % 2) for bit in bits]
    line = [{"cp": row * ranks + partner} for partner in partners]

    def peer(s):
        other = row
        bit = 1
        while bit <= s:
            if s & bit:
                other = other + bit - 2 * bit * ((other // bit) % 2)
            bit *= 2
        return other

    def at_column(s, t):
        return {"cp": peer(s) * ranks + rank, "tp": (tp + t) % tps}

    greet(
        [{"cp": (me + d) % parts} for d in range(1, parts)]
        + [at_column(s, t) for s in range(heads) for t in range(1, tps)]
    )

    def span(ref, start, size, step):
        return ref.at[pl.ds(pl.multiple_of(start, step), size), pl.ds(0, HEAD_SIZE)]

    def cut(ref, head):
        return ref.at[:, pl.ds(pl.multiple_of(head * HEAD_SIZE, HEAD_SIZE), HEAD_SIZE)]

    def place(a, index):
        target = k2 if a % 2 == 0 else v_land
        if a < 2:
            return span(target, fresh + index * block, block, block)
        return span(target, index * (tps * few), tps * few, tps * few)

    shifts = range(heads)
    started = []

    def go(copy):
        copy.start()
        started.append(copy)
        return copy

    arrived = {}
    for s in shifts:
        for a, source in enumerate((cache_k, cache_v)):
            piece = cut(source, peer(s))
            if s == 0:
                copy = pltpu.make_async_copy(piece, place(a, me), z_recv.at[a, s])
                copy.start()
                arrived[a, s] = [copy.wait]
            else:
                copy = go(
                    remote(piece, place(a, me), z_send.at[a, s], z_recv.at[a, s], at_column(s, 0))
                )
                arrived[a, s] = [copy.wait_recv]
        for a, source in enumerate((fresh_k, fresh_v)):
            waits = []
            for t in range(tps):
                to = at_column(s, t)
                piece = cut(source, to["tp"] * heads + peer(s))
                target = span((k2, v_land)[a], me * (tps * few) + tp * few, few, few)
                if s == 0 and t == 0:
                    copy = pltpu.make_async_copy(piece, target, fresh_recv.at[a, s, t])
                    copy.start()
                    waits.append(copy.wait)
                else:
                    copy = go(
                        remote(
                            piece, target, fresh_send.at[a, s, t], fresh_recv.at[a, s, t], to
                        )
                    )
                    waits.append(copy.wait_recv)
            arrived[2 + a, s] = waits

    def query_copy(g, s, t, local):
        to = at_column(s, t)
        start = (to["tp"] * heads + peer(s)) * own_columns + g * width
        source = query.at[:, pl.ds(pl.multiple_of(start, width), width)]
        target = q_land.at[g, pl.ds(pl.multiple_of((row * tps + tp) * few, few), few), :]
        if local:
            return pltpu.make_async_copy(source, target, q_recv.at[g, 0])
        return remote(source, target, q_send.at[g, s * tps + t], q_recv.at[g, s * tps + t], to)

    routes = [(s, t) for s in shifts for t in range(tps)]

    def send_query(g, _):
        for s, t in routes:
            query_copy(g, s, t, s == 0 and t == 0).start()
        return 0

    lax.fori_loop(0, steps, send_query, 0)

    order = (2, 3, 0, 1)
    held = [((a, s), a, s, rank) for s in shifts for a in order]
    for level, partner in enumerate(partners):
        send, receive = rank_sems[2 * level], rank_sems[2 * level + 1]
        other = []
        for number, (key, a, s, owner) in enumerate(held):
            for wait in arrived.pop(key, ()):
                wait()
            index = peer(s) * ranks + owner
            copy = go(
                remote(
                    place(a, index), place(a, index), send.at[number], receive.at[number], line[level]
                )
            )
            bit = bits[level]
            name = (a, s, level + 1, number)
            arrived[name] = [copy.wait_recv]
            other.append((name, a, s, owner + bit - 2 * bit * ((owner // bit) % 2)))
        held = held + other
    twins = []

    def twin(number, start, size):
        copy = pltpu.make_async_copy(
            span(k2, start, size, size),
            k2.at[pl.ds(pl.multiple_of(start, size), size), pl.ds(HEAD_SIZE, HEAD_SIZE)],
            twin_sem.at[number],
        )
        copy.start()
        twins.append(copy)

    lane = lax.broadcasted_iota(jnp.int32, (rows, rows), 1)
    sorted_row = lax.broadcasted_iota(jnp.int32, (rows, rows), 0)

    def natural(at):
        many = tps * few
        stripe = many // parts
        inside = jnp.zeros(at.shape, jnp.int32)
        for r in range(parts):
            inside = jnp.where(at // share == owner_ref[r], r * stripe, inside)
        return at % share // stripe, inside + at % stripe

    z, inside = natural(sorted_row)
    pick_ref[...] = (z * (tps * few) + inside == lane).astype(jnp.float32).astype(jnp.bfloat16)

    for key, a, s, owner in held:
        for wait in arrived.pop(key, ()):
            wait()
        index = peer(s) * ranks + owner
        if a == 0:
            twin(len(twins), fresh + index * block, block)
        elif a == 2:
            twin(len(twins), index * (tps * few), tps * few)

    eye = (
        lax.broadcasted_iota(jnp.int32, (HEAD_SIZE, HEAD_SIZE), 0)
        == lax.broadcasted_iota(jnp.int32, (HEAD_SIZE, HEAD_SIZE), 1)
    ).astype(jnp.bfloat16)

    def prepare(b, _):
        at = pl.multiple_of(b * chunk, chunk)
        vt[:, pl.ds(at, chunk)] = lax.dot_general(
            eye, v_land[pl.ds(at, chunk), :], dn, preferred_element_type=jnp.float32
        ).astype(jnp.bfloat16)
        return 0

    lax.fori_loop(0, keys // chunk, prepare, 0)
    for copy in twins:
        copy.wait()

    slabs = ((s0, t0), (s1, t1))

    def score(at, slab, h, mask):
        s_ref, t_ref = slabs[slab]
        s = jnp.dot(
            k2[pl.ds(at, chunk), :],
            q2[:, h * rows : (h + 1) * rows],
            preferred_element_type=jnp.float32,
        )
        if mask is not None:
            s = jnp.where(mask, s, NEG)
        s_ref[h] = s
        t_ref[h] = jnp.max(s, axis=0, keepdims=True)

    def soften(at, slab, h, first):
        s_ref, t_ref = slabs[slab]
        top = t_ref[h]
        m_new = top if first else jnp.maximum(m_ref[h], top)
        p = jnp.exp2(s_ref[h] - m_new)
        total = jnp.sum(p, axis=0, keepdims=True)
        o = jnp.dot(
            vt[:, pl.ds(at, chunk)], p.astype(jnp.bfloat16), preferred_element_type=jnp.float32
        )
        if first:
            l_ref[h] = total
            acc_ref[h] = o
        else:
            f = jnp.exp2(m_ref[h] - m_new)
            l_ref[h] = f * l_ref[h] + total
            acc_ref[h] = f * acc_ref[h] + o
        m_ref[h] = m_new

    def output_copy(g, d):
        to = (me + d) % parts
        columns = pl.ds(pl.multiple_of(g * width, width), width)
        source = o_buf.at[pl.ds(pl.multiple_of(to * share, share), share), columns]
        target = out.at[
            pl.ds(pl.multiple_of(rank * share, share), share),
            pl.ds(pl.multiple_of(row * own_columns + g * width, width), width),
        ]
        if d == 0:
            return pltpu.make_async_copy(source, target, o_recv.at[g, 0])
        return remote(source, target, o_send.at[g, d], o_recv.at[g, d], {"cp": to})

    def send_output(g):
        for d in range(parts):
            output_copy(g, d).start()

    number = fresh // chunk
    units = slots // chunk
    group = 4
    index = lax.broadcasted_iota(jnp.int32, (chunk, rows), 0)
    sure = (units // 2 - 1) // group

    def step(g, _):
        for s, t in routes:
            if s == 0 and t == 0:
                query_copy(g, s, t, True).wait()
            else:
                query_copy(g, s, t, False).wait_recv()
        for h in range(per_step):
            x = jnp.dot(
                pick_ref[...],
                q_land[g, :, h * HEAD_SIZE : (h + 1) * HEAD_SIZE],
                preferred_element_type=jnp.float32,
            )
            x = x.T * EXPONENT
            hi = x.astype(jnp.bfloat16)
            q2[:HEAD_SIZE, h * rows : (h + 1) * rows] = hi
            q2[HEAD_SIZE:, h * rows : (h + 1) * rows] = (x - hi.astype(jnp.float32)).astype(
                jnp.bfloat16
            )

        @pl.when(g > 0)
        def _():
            send_output(g - 1)

        z, inside = natural(lax.broadcasted_iota(jnp.int32, (1, rows), 1))
        nat = (z * ranks + rank) * (tps * few) + inside
        for h in range(per_step):
            score(0, 0, h, index <= nat)
        for c in range(number):
            for h in range(per_step):
                if c + 1 < number:
                    score((c + 1) * chunk, (c + 1) % 2, h, index + (c + 1) * chunk <= nat)
                else:
                    score(fresh, 0, h, None)
                soften(c * chunk, c % 2, h, c == 0)

        def batch(masked, j):
            for u in range(group):
                slot = (j * group + u) * chunk
                after = slot + chunk
                mask = index + after < plen_ref[0] if masked else None
                for h in range(per_step):
                    score(pl.multiple_of(fresh + after, chunk), (u + 1) % 2, h, mask)
                    soften(pl.multiple_of(fresh + slot, chunk), u % 2, h, False)
            return 0

        def finish_head(h):
            columns = pl.ds(pl.multiple_of(g * width + h * HEAD_SIZE, HEAD_SIZE), HEAD_SIZE)
            o_buf[:, columns] = (acc_ref[h] / l_ref[h]).T.astype(o_buf.dtype)

        if sure == 1:
            batch(False, 0)
        else:
            lax.fori_loop(0, sure, lambda j, _: batch(False, j), 0)
        lax.fori_loop(sure, units // group - 1, lambda j, _: batch(True, j), 0)
        for u in range(units - group, units):
            for h in range(per_step):
                if u + 1 < units:
                    after = (u + 1) * chunk
                    score(fresh + after, (u + 1) % 2, h, index + after < plen_ref[0])
                soften(fresh + u * chunk, u % 2, h, False)
                if u + 1 == units:
                    finish_head(h)
        return 0

    lax.fori_loop(0, steps, step, 0)
    send_output(steps - 1)

    def finish(g, _):
        for s, t in routes:
            if s != 0 or t != 0:
                query_copy(g, s, t, False).wait_send()
        for d in range(parts):
            output_copy(g, d).wait()
        return 0

    for copy in started:
        copy.wait_send()
    lax.fori_loop(0, steps, finish, 0)


def fused(
    plen, owner, query, fresh_k, fresh_v, cache_k, cache_v, heads, ranks, tps, per_step, chunk
):
    parts = heads * ranks
    few, block = fresh_k.shape[0], cache_k.shape[0]
    fresh = parts * tps * few
    keys = fresh + parts * block
    rows = heads * tps * few
    width = per_step * HEAD_SIZE
    wide = per_step * rows
    own_columns = query.shape[1] // (tps * heads)
    steps = own_columns // width
    rank_sems = []
    count = 4 * heads
    size = ranks
    while size > 1:
        rank_sems += [pltpu.SemaphoreType.DMA((count,))] * 2
        count *= 2
        size //= 2
    dma = pltpu.SemaphoreType.DMA
    b16, f32 = jnp.bfloat16, jnp.float32
    return pl.pallas_call(
        functools.partial(fused_kernel, (heads, ranks, tps, per_step, chunk)),
        out_shape=jax.ShapeDtypeStruct((tps * few, heads * own_columns), b16),
        in_specs=[pl.BlockSpec(memory_space=pltpu.SMEM)] * 2
        + [pl.BlockSpec(memory_space=pl.ANY)] * 5,
        out_specs=pl.BlockSpec(memory_space=pl.ANY),
        scratch_shapes=[
            pltpu.VMEM((keys, 2 * HEAD_SIZE), b16),
            pltpu.VMEM((keys, HEAD_SIZE), b16),
            pltpu.VMEM((HEAD_SIZE, keys), b16),
            pltpu.VMEM((steps, rows, width), b16),
            pltpu.VMEM((rows, own_columns), b16),
            pltpu.VMEM((2 * HEAD_SIZE, wide), b16),
            pltpu.VMEM((rows, rows), b16),
            pltpu.VMEM((per_step, chunk, rows), f32),
            pltpu.VMEM((per_step, chunk, rows), f32),
            pltpu.VMEM((per_step, 1, rows), f32),
            pltpu.VMEM((per_step, 1, rows), f32),
            pltpu.VMEM((per_step, 1, rows), f32),
            pltpu.VMEM((per_step, 1, rows), f32),
            pltpu.VMEM((per_step, HEAD_SIZE, rows), f32),
            dma((2, heads, tps)),
            dma((2, heads, tps)),
            dma((2, heads)),
            dma((2, heads)),
            dma((steps, heads * tps)),
            dma((steps, heads * tps)),
            dma((steps, parts)),
            dma((steps, parts)),
            dma((2 * parts,)),
        ]
        + rank_sems,
        compiler_params=pltpu.CompilerParams(
            collective_id=1, has_side_effects=True, vmem_limit_bytes=56 * 1024 * 1024
        ),
        cost_estimate=pl.CostEstimate(
            flops=4 * rows * own_columns * keys, bytes_accessed=100000000, transcendentals=0
        ),
    )(plen, owner, query, fresh_k, fresh_v, cache_k, cache_v)


def exchanged(
    query,
    fresh_key_rows,
    fresh_value_rows,
    cached_key_rows,
    cached_value_rows,
    prefix_len,
    stripe_owner,
    per_step,
    chunk,
):
    parts, tps = lax.axis_size("cp"), lax.axis_size("tp")
    heads = cached_key_rows.shape[1] // HEAD_SIZE
    ranks = parts // heads
    landed = fused(
        prefix_len,
        stripe_owner,
        query,
        fresh_key_rows,
        fresh_value_rows,
        cached_key_rows,
        cached_value_rows,
        heads,
        ranks,
        tps,
        per_step,
        chunk,
    )
    rows = landed.shape[0]
    stripe = rows // parts
    order = jnp.arange(rows, dtype=jnp.int32).reshape(ranks, heads, stripe)
    order = order.transpose(1, 0, 2).reshape(rows)
    move = (order[:, None] == jnp.arange(rows, dtype=jnp.int32)[None, :]).astype(jnp.bfloat16)
    return jnp.dot(move, landed, preferred_element_type=jnp.float32).astype(jnp.bfloat16)


def plain(
    query, fresh_key_rows, fresh_value_rows, cached_key_rows, cached_value_rows, prefix_len, inverse
):
    parts = lax.axis_size("cp")
    me = lax.axis_index("cp")
    heads = cached_key_rows.shape[1] // HEAD_SIZE
    ranks = parts // heads
    tps = lax.axis_size("tp")
    q_columns = query.shape[1] // tps // heads
    columns = [[h * ranks + r for h in range(heads)] for r in range(ranks)]
    lines = [[h * ranks + r for r in range(ranks)] for h in range(heads)]

    def split_heads(array, axis_name="cp"):
        if heads == 1:
            return array
        return lax.all_to_all(
            array, axis_name, split_axis=1, concat_axis=0, axis_index_groups=columns, tiled=True
        )

    def collect(array):
        block = array.shape[0]
        mine = split_heads(array)
        everything = lax.all_gather(mine, "cp", axis_index_groups=lines, tiled=True)
        return (
            everything.reshape(ranks, heads, block, HEAD_SIZE)
            .transpose(1, 0, 2, 3)
            .reshape(parts * block, HEAD_SIZE)
        )

    q_local = lax.all_to_all(query, "tp", split_axis=1, concat_axis=0, tiled=True)
    rows = q_local.shape[0]
    stripe = rows // parts
    by_rank = inverse.reshape(heads, ranks).T.reshape(-1)
    wanted = (by_rank[:, None] * stripe + jnp.arange(stripe, dtype=jnp.int32)[None, :]).reshape(-1)
    pick = (wanted[:, None] == jnp.arange(rows, dtype=jnp.int32)[None, :]).astype(jnp.bfloat16)
    q_sorted = jnp.dot(pick, q_local, preferred_element_type=jnp.float32).astype(jnp.bfloat16)
    q_out = (
        q_sorted.reshape(ranks, heads * stripe, heads, q_columns)
        .transpose(2, 0, 1, 3)
        .reshape(parts * heads * stripe, q_columns)
    )
    q_mine = lax.all_to_all(q_out, "cp", split_axis=0, concat_axis=0, tiled=True)
    own = [
        lax.all_to_all(array, "tp", split_axis=1, concat_axis=0, tiled=True)
        for array in (fresh_key_rows, fresh_value_rows)
    ]
    cache_k, cache_v, fresh_k, fresh_v = (
        collect(array) for array in (cached_key_rows, cached_value_rows, *own)
    )
    residues = jnp.take(by_rank.reshape(ranks, heads), me % ranks, axis=0)
    nat = (
        jnp.arange(parts, dtype=jnp.int32)[:, None, None] * rows
        + residues[None, :, None] * stripe
        + jnp.arange(stripe, dtype=jnp.int32)[None, None, :]
    ).reshape(1, -1)
    per_step = max(1, min(q_columns // HEAD_SIZE, 512 // nat.shape[1]))
    nat = jnp.tile(nat, (1, per_step))
    done = attend(q_mine, nat, fresh_k, fresh_v, cache_k, cache_v, prefix_len)
    done = (
        done.reshape(parts, heads, stripe, q_columns)
        .transpose(1, 0, 2, 3)
        .reshape(heads * rows, q_columns)
    )
    if heads == 1:
        return done
    split = done.reshape(heads, rows, q_columns)
    back = lax.all_to_all(
        split, "cp", split_axis=0, concat_axis=0, axis_index_groups=columns, tiled=True
    )
    return back.transpose(1, 0, 2).reshape(rows, heads * q_columns)


def shards(
    query,
    fresh_key_rows,
    fresh_value_rows,
    cached_key_rows,
    cached_value_rows,
    prefix_len,
    stripe_owner,
):
    parts, tps = lax.axis_size("cp"), lax.axis_size("tp")
    heads = cached_key_rows.shape[1] // HEAD_SIZE
    ranks = parts // heads
    arrays = (query, fresh_key_rows, fresh_value_rows, cached_key_rows, cached_value_rows)
    rows = heads * tps * fresh_key_rows.shape[0]
    fresh = rows * ranks
    slots = parts * cached_key_rows.shape[0]
    group = query.shape[1] // (tps * heads * HEAD_SIZE)
    per_step, chunk = math.gcd(4, group), 512
    fits = (
        heads > 1
        and heads & (heads - 1) == 0
        and ranks & (ranks - 1) == 0
        and rows % (8 * parts) == 0
        and rows % HEAD_SIZE == 0
        and rows <= 512
        and fresh % (2 * chunk) == 0
        and slots % (8 * chunk) == 0
    )
    if fits:
        return exchanged(*arrays, prefix_len, stripe_owner, per_step, chunk)
    order = jnp.arange(parts, dtype=jnp.int32)
    inverse = jnp.sum(jnp.where(stripe_owner[None, :] == order[:, None], order[None, :], 0), axis=1)
    return plain(*arrays, prefix_len, inverse)


def solution(mesh):
    return jax.shard_map(
        shards,
        mesh=mesh,
        in_specs=(
            P(("cp", "tp"), None),
            P(("cp", "tp"), None),
            P(("cp", "tp"), None),
            P("cp", "tp"),
            P("cp", "tp"),
            P(),
            P(),
        ),
        out_specs=P("cp", "tp"),
        check_vma=False,
    )
```

```python
import functools
import math

import jax
import jax.numpy as jnp
from jax import lax
from jax.experimental import pallas as pl
from jax.experimental.pallas import tpu as pltpu
from jax.sharding import PartitionSpec as P

HEAD_SIZE = 128
NEG = -1e30
EXPONENT = HEAD_SIZE ** (-0.5) * math.log2(math.e)


def attend_kernel(dims, plen_ref, q_ref, nat_ref, fresh_k, fresh_v, cache_k, cache_v, out_ref,
                  k2, vt, q2, s0, s1, m_ref, l_ref, acc_ref):
    per_step, chunk = dims
    rows = q_ref.shape[0]
    wide = rows * per_step
    plen = plen_ref[0]
    fresh, slots = fresh_k.shape[0], cache_k.shape[0]
    dn = (((1,), (1,)), ((), ()))

    @pl.when(pl.program_id(0) == 0)
    def _():
        eye = (lax.broadcasted_iota(jnp.int32, (HEAD_SIZE, HEAD_SIZE), 0)
               == lax.broadcasted_iota(jnp.int32, (HEAD_SIZE, HEAD_SIZE), 1)).astype(jnp.bfloat16)
        step = min(512, fresh)

        def prepare(source_k, source_v, base, count):
            def body(b, _):
                at = pl.multiple_of(b * step, step)
                to = pl.multiple_of(base + b * step, step)
                k = source_k[pl.ds(at, step), :]
                k2[pl.ds(to, step), :HEAD_SIZE] = k
                k2[pl.ds(to, step), HEAD_SIZE:] = k
                v = source_v[pl.ds(at, step), :]
                vt[:, pl.ds(to, step)] = lax.dot_general(
                    eye, v, dn, preferred_element_type=jnp.float32).astype(jnp.bfloat16)
                return 0
            lax.fori_loop(0, count // step, body, 0)
        prepare(fresh_k, fresh_v, 0, fresh)
        prepare(cache_k, cache_v, fresh, slots)

    for g in range(per_step):
        x = q_ref[:, g * HEAD_SIZE:(g + 1) * HEAD_SIZE].astype(jnp.float32) * EXPONENT
        x = x.T
        hi = x.astype(jnp.bfloat16)
        q2[:HEAD_SIZE, g * rows:(g + 1) * rows] = hi
        q2[HEAD_SIZE:, g * rows:(g + 1) * rows] = (x - hi.astype(jnp.float32)).astype(jnp.bfloat16)

    def score(at, s):
        s[...] = jnp.dot(k2[pl.ds(at, chunk), :], q2[...], preferred_element_type=jnp.float32)

    def soften(at, s_ref, mask, first):
        s = s_ref[...]
        if mask is not None:
            s = jnp.where(mask, s, NEG)
        top = jnp.max(s, axis=0, keepdims=True)
        m_new = top if first else jnp.maximum(m_ref[...], top)
        p = jnp.exp2(s - m_new)
        total = jnp.sum(p, axis=0, keepdims=True)
        o = jnp.dot(vt[:, pl.ds(at, chunk)], p.astype(jnp.bfloat16), preferred_element_type=jnp.float32)
        if first:
            l_ref[...] = total
            acc_ref[...] = o
        else:
            f = jnp.exp2(m_ref[...] - m_new)
            l_ref[...] = f * l_ref[...] + total
            acc_ref[...] = f * acc_ref[...] + o
        m_ref[...] = m_new

    bufs = (s0, s1)
    number = fresh // chunk
    assert number % 2 == 0
    nat = nat_ref[...]
    index = lax.broadcasted_iota(jnp.int32, (chunk, wide), 0)
    score(0, s0)
    for c in range(number):
        score((c + 1) * chunk, bufs[(c + 1) % 2])
        soften(c * chunk, bufs[c % 2], index + c * chunk <= nat, c == 0)

    pairs = (plen + 2 * chunk - 1) // (2 * chunk)

    def body(j, _):
        at = pl.multiple_of(fresh + 2 * j * chunk, chunk)
        score(pl.multiple_of(at + chunk, chunk), s1)
        soften(at, s0, None, False)
        score(pl.multiple_of(at + 2 * chunk, chunk), s0)
        soften(pl.multiple_of(at + chunk, chunk), s1, None, False)
        return 0
    lax.fori_loop(0, pairs - 1, body, 0)
    slot = 2 * (pairs - 1) * chunk
    at = pl.multiple_of(fresh + slot, chunk)
    score(pl.multiple_of(at + chunk, chunk), s1)
    soften(at, s0, index + slot < plen, False)
    soften(pl.multiple_of(at + chunk, chunk), s1, index + (slot + chunk) < plen, False)

    done = acc_ref[...] / l_ref[...]
    for g in range(per_step):
        out_ref[:, g * HEAD_SIZE:(g + 1) * HEAD_SIZE] = done[:, g * rows:(g + 1) * rows].T.astype(out_ref.dtype)


def attend(q, nat, fresh_k, fresh_v, cache_k, cache_v, prefix_len, chunk=512):
    rows, columns = q.shape
    per_step = nat.shape[1] // rows
    width = per_step * HEAD_SIZE
    wide = per_step * rows
    fresh, slots = fresh_k.shape[0], cache_k.shape[0]
    whole = lambda i, *_: (0, 0)
    keys = fresh + slots
    return pl.pallas_call(
        functools.partial(attend_kernel, (per_step, chunk)),
        out_shape=jax.ShapeDtypeStruct((rows, columns), jnp.bfloat16),
        grid_spec=pltpu.PrefetchScalarGridSpec(
            num_scalar_prefetch=1,
            grid=(columns // width,),
            in_specs=[
                pl.BlockSpec((rows, width), lambda i, *_: (0, i)),
                pl.BlockSpec((1, wide), whole),
                pl.BlockSpec((fresh, HEAD_SIZE), whole),
                pl.BlockSpec((fresh, HEAD_SIZE), whole),
                pl.BlockSpec((slots, HEAD_SIZE), whole),
                pl.BlockSpec((slots, HEAD_SIZE), whole),
            ],
            out_specs=pl.BlockSpec((rows, width), lambda i, *_: (0, i)),
            scratch_shapes=[
                pltpu.VMEM((keys, 2 * HEAD_SIZE), jnp.bfloat16),
                pltpu.VMEM((HEAD_SIZE, keys), jnp.bfloat16),
                pltpu.VMEM((2 * HEAD_SIZE, wide), jnp.bfloat16),
                pltpu.VMEM((chunk, wide), jnp.float32),
                pltpu.VMEM((chunk, wide), jnp.float32),
                pltpu.VMEM((1, wide), jnp.float32),
                pltpu.VMEM((1, wide), jnp.float32),
                pltpu.VMEM((HEAD_SIZE, wide), jnp.float32),
            ],
        ),
        compiler_params=pltpu.CompilerParams(vmem_limit_bytes=56 * 1024 * 1024),
        cost_estimate=pl.CostEstimate(flops=4*rows*columns*keys, bytes_accessed=4 * keys*HEAD_SIZE, transcendentals=0),
    )(prefix_len, q, nat, fresh_k, fresh_v, cache_k, cache_v)


def remote(source, target, send, receive, device):
    return pltpu.make_async_remote_copy(
        src_ref=source,
        dst_ref=target,
        send_sem=send,
        recv_sem=receive,
        device_id=device,
        device_id_type=pl.DeviceIdType.MESH,
    )


def greet(devices):
    barrier = pltpu.get_barrier_semaphore()
    for device in devices:
        pl.semaphore_signal(
            barrier, inc=1, device_id=device, device_id_type=pl.DeviceIdType.MESH
        )
    pl.semaphore_wait(barrier, len(devices))


def fused_kernel(
    sizes,
    plen_ref,
    owner_ref,
    query,
    fresh_k,
    fresh_v,
    cache_k,
    cache_v,
    out,
    k2,
    v_land,
    vt,
    q_land,
    o_buf,
    q2,
    pick_ref,
    s0,
    s1,
    t0,
    t1,
    m_ref,
    l_ref,
    acc_ref,
    fresh_send,
    fresh_recv,
    z_send,
    z_recv,
    q_send,
    q_recv,
    o_send,
    o_recv,
    twin_sem,
    *rank_sems,
):
    heads, ranks, tps, per_step, chunk = sizes
    parts = heads * ranks
    me, tp = lax.axis_index("cp"), lax.axis_index("tp")
    row, rank = me // ranks, me % ranks
    few = fresh_k.shape[0]
    block = cache_k.shape[0]
    fresh = parts * tps * few
    keys = k2.shape[0]
    slots = keys - fresh
    steps, rows, width = q_land.shape
    own_columns = steps * width
    wide = per_step * rows
    share = rows // parts
    dn = (((1,), (1,)), ((), ()))

    bits = []
    bit = ranks // 2
    while bit:
        bits.append(bit)
        bit //= 2
    partners = [rank + bit - 2 * bit * ((rank // bit) % 2) for bit in bits]
    line = [{"cp": row * ranks + partner} for partner in partners]

    def peer(s):
        other = row
        bit = 1
        while bit < heads:
            other = other + (s // bit) % 2 * (bit - 2 * bit * ((other // bit) % 2))
            bit *= 2
        return other

    def at_column(s, t):
        return {"cp": peer(s) * ranks + rank, "tp": (tp + t) % tps}

    greet(
        [{"cp": (me + d) % parts} for d in range(1, parts)]
        + [at_column(s, t) for s in range(heads) for t in range(1, tps)]
    )

    def span(ref, start, size, step):
        return ref.at[pl.ds(pl.multiple_of(start, step), size), pl.ds(0, HEAD_SIZE)]

    def cut(ref, head):
        return ref.at[:, pl.ds(pl.multiple_of(head * HEAD_SIZE, HEAD_SIZE), HEAD_SIZE)]

    def place(a, index):
        target = k2 if a % 2 == 0 else v_land
        if a < 2:
            return span(target, fresh + index * block, block, block)
        return span(target, index * (tps * few), tps * few, tps * few)

    shifts = range(heads)
    started = []

    def go(copy):
        copy.start()
        started.append(copy)
        return copy

    arrived = {}
    for s in shifts:
        for a, source in enumerate((fresh_k, fresh_v)):
            waits = []
            for t in range(tps):
                to = at_column(s, t)
                piece = cut(source, to["tp"] * heads + peer(s))
                target = span((k2, v_land)[a], me * (tps * few) + tp * few, few, few)
                if s == 0 and t == 0:
                    copy = pltpu.make_async_copy(piece, target, fresh_recv.at[a, s, t])
                    copy.start()
                    waits.append(copy.wait)
                else:
                    copy = go(
                        remote(
                            piece, target, fresh_send.at[a, s, t], fresh_recv.at[a, s, t], to
                        )
                    )
                    waits.append(copy.wait_recv)
            arrived[2 + a, s, 0] = waits
    for s in shifts:
        for a, source in enumerate((cache_k, cache_v)):
            piece = cut(source, peer(s))
            if s == 0:
                copy = pltpu.make_async_copy(piece, place(a, me), z_recv.at[a, s])
                copy.start()
                arrived[a, s, 0] = [copy.wait]
            else:
                copy = go(
                    remote(piece, place(a, me), z_send.at[a, s], z_recv.at[a, s], at_column(s, 0))
                )
                arrived[a, s, 0] = [copy.wait_recv]

    def query_copy(g, s, t, local):
        to = at_column(s, t)
        start = (to["tp"] * heads + peer(s)) * own_columns + g * width
        source = query.at[:, pl.ds(pl.multiple_of(start, width), width)]
        target = q_land.at[g, pl.ds(pl.multiple_of((row * tps + tp) * few, few), few), :]
        if local:
            return pltpu.make_async_copy(source, target, q_recv.at[g, 0])
        return remote(source, target, q_send.at[g, s * tps + t], q_recv.at[g, s * tps + t], to)

    routes = [(s, t) for s in shifts for t in range(tps)]

    def send_query(g, _):
        for s, t in routes:
            query_copy(g, s, t, s == 0 and t == 0).start()
        return 0

    lax.fori_loop(0, steps, send_query, 0)

    relays, held = {}, {}
    for s in shifts:
        for a in range(4):
            mine = [((a, s, 0), rank)]
            for level, partner in enumerate(partners):
                send, receive = rank_sems[2 * level], rank_sems[2 * level + 1]
                bit = bits[level]
                other = []
                for k, (key, owner) in enumerate(mine):
                    number = (s * 4 + a) * 2**level + k
                    piece = place(a, peer(s) * ranks + owner)
                    copy = remote(piece, piece, send.at[number], receive.at[number], line[level])
                    started.append(copy)
                    relays.setdefault((a // 2, s, level), []).append((key, copy))
                    name = (a, s, level + 1, k)
                    arrived[name] = [copy.wait_recv]
                    other.append((name, owner + bit - 2 * bit * ((owner // bit) % 2)))
                mine = mine + other
            for key, owner in mine:
                index = peer(s) * ranks + owner
                held.setdefault((a // 2, s), []).append((key, a, index))
    twin_copies = {}
    for kind, s in held:
        for key, a, index in held[kind, s]:
            if a % 2 == 0:
                size = tps * few if kind else block
                start = index * size + (0 if kind else fresh)
                twin_copies[key] = pltpu.make_async_copy(
                    span(k2, start, size, size),
                    k2.at[pl.ds(pl.multiple_of(start, size), size), pl.ds(HEAD_SIZE, HEAD_SIZE)],
                    twin_sem.at[len(twin_copies)],
                )

    def relay(kind, s, level):
        for key, copy in relays[kind, s, level]:
            if key[2] == level:
                for wait in arrived[key]:
                    wait()
            copy.start()

    levels = len(partners)
    waves = sorted(((s, l) for s in shifts for l in range(levels)), key=lambda w: (sum(w), w[1]))
    early = [w for w in waves if sum(w) < heads or heads <= 2]
    late = [w for w in waves if w not in early]
    for number, (s, level) in enumerate(early):
        relay(0, s, level)
        if s == 0:
            for other in shifts:
                relay(1, other, level)

    lane = lax.broadcasted_iota(jnp.int32, (rows, rows), 1)
    sorted_row = lax.broadcasted_iota(jnp.int32, (rows, rows), 0)

    def natural(at):
        many = tps * few
        stripe = many // parts
        inside = jnp.zeros(at.shape, jnp.int32)
        for r in range(parts):
            inside = jnp.where(at // share == owner_ref[r], r * stripe, inside)
        return at % share // stripe, inside + at % stripe

    z, inside = natural(sorted_row)
    pick_ref[...] = (z * (tps * few) + inside == lane).astype(jnp.float32).astype(jnp.bfloat16)

    eye = (
        lax.broadcasted_iota(jnp.int32, (HEAD_SIZE, HEAD_SIZE), 0)
        == lax.broadcasted_iota(jnp.int32, (HEAD_SIZE, HEAD_SIZE), 1)
    ).astype(jnp.bfloat16)

    def complete(kind, s, base, count):
        items = held[kind, s]
        for key, a, index in items:
            if key[2] == levels:
                for wait in arrived[key]:
                    wait()
            if key in twin_copies:
                twin_copies[key].start()

        def prepare(b, _):
            at = pl.multiple_of(base + b * chunk, chunk)
            vt[:, pl.ds(at, chunk)] = lax.dot_general(
                eye, v_land[pl.ds(at, chunk), :], dn, preferred_element_type=jnp.float32
            ).astype(jnp.bfloat16)
            return 0

        lax.fori_loop(0, count // chunk, prepare, 0)
        for key, a, index in items:
            if key in twin_copies:
                twin_copies[key].wait()

    for s in shifts:
        complete(1, s, 0, fresh if s == heads - 1 else 0)
    part = ranks * block
    for s in range(2):
        complete(0, s, fresh + peer(s) * part, part)

    slabs = ((s0, t0), (s1, t1))

    def score(at, slab, h, mask):
        s_ref, t_ref = slabs[slab]
        s = jnp.dot(
            k2[pl.ds(at, chunk), :],
            q2[:, h * rows : (h + 1) * rows],
            preferred_element_type=jnp.float32,
        )
        if mask is not None:
            s = jnp.where(mask, s, NEG)
        s_ref[h] = s
        t_ref[h] = jnp.max(s, axis=0, keepdims=True)

    def soften(at, slab, h, first):
        s_ref, t_ref = slabs[slab]
        top = t_ref[h]
        m_new = top if first else jnp.maximum(m_ref[h], top)
        p = jnp.exp2(s_ref[h] - m_new)
        total = jnp.sum(p, axis=0, keepdims=True)
        o = jnp.dot(
            vt[:, pl.ds(at, chunk)], p.astype(jnp.bfloat16), preferred_element_type=jnp.float32
        )
        if first:
            l_ref[h] = total
            acc_ref[h] = o
        else:
            f = jnp.exp2(m_ref[h] - m_new)
            l_ref[h] = f * l_ref[h] + total
            acc_ref[h] = f * acc_ref[h] + o
        m_ref[h] = m_new

    def output_copy(g, d):
        to = (me + d) % parts
        columns = pl.ds(pl.multiple_of(g * width, width), width)
        source = o_buf.at[pl.ds(pl.multiple_of(to * share, share), share), columns]
        target = out.at[
            pl.ds(pl.multiple_of(rank * share, share), share),
            pl.ds(pl.multiple_of(row * own_columns + g * width, width), width),
        ]
        if d == 0:
            return pltpu.make_async_copy(source, target, o_recv.at[g, 0])
        return remote(source, target, o_send.at[g, d], o_recv.at[g, d], {"cp": to})

    def send_output(g):
        for d in range(parts):
            output_copy(g, d).start()

    number = fresh // chunk
    units = slots // chunk
    group = part // chunk
    index = lax.broadcasted_iota(jnp.int32, (chunk, rows), 0)

    def step(g, _):
        for s, t in routes:
            if s == 0 and t == 0:
                query_copy(g, s, t, True).wait()
            else:
                query_copy(g, s, t, False).wait_recv()
        for h in range(per_step):
            x = jnp.dot(
                pick_ref[...],
                q_land[g, :, h * HEAD_SIZE : (h + 1) * HEAD_SIZE],
                preferred_element_type=jnp.float32,
            )
            x = x.T * EXPONENT
            hi = x.astype(jnp.bfloat16)
            q2[:HEAD_SIZE, h * rows : (h + 1) * rows] = hi
            q2[HEAD_SIZE:, h * rows : (h + 1) * rows] = (x - hi.astype(jnp.float32)).astype(
                jnp.bfloat16
            )

        @pl.when(g > 0)
        def _():
            send_output(g - 1)

        def base_of(s):
            return pl.multiple_of(fresh + peer(s) * part, chunk)

        z, inside = natural(lax.broadcasted_iota(jnp.int32, (1, rows), 1))
        nat = (z * ranks + rank) * (tps * few) + inside
        for h in range(per_step):
            score(0, 0, h, index <= nat)
        for c in range(number):
            for h in range(per_step):
                if c + 1 < number:
                    score((c + 1) * chunk, (c + 1) % 2, h, index + (c + 1) * chunk <= nat)
                else:
                    score(base_of(0), 0, h, index + peer(0) * part < plen_ref[0])
                soften(c * chunk, c % 2, h, c == 0)

        def batch(j, last):
            here = peer(j) * part
            beyond = None if last else peer(j + 1) * part
            for u in range(group):
                slot = here + u * chunk
                after = slot + chunk if u + 1 < group else beyond
                for h in range(per_step):
                    if after is not None:
                        score(
                            pl.multiple_of(fresh + after, chunk),
                            (u + 1) % 2,
                            h,
                            index + after < plen_ref[0],
                        )
                    soften(pl.multiple_of(fresh + slot, chunk), u % 2, h, False)
                    if after is None:
                        finish_head(h)
            return 0

        def finish_head(h):
            columns = pl.ds(pl.multiple_of(g * width + h * HEAD_SIZE, HEAD_SIZE), HEAD_SIZE)
            o_buf[:, columns] = (acc_ref[h] / l_ref[h]).T.astype(o_buf.dtype)

        batch(0, False)

        def middle(j, _):
            for s in range(2, heads):

                @pl.when((g == 0) & (j == s - 1))
                def _():
                    if s == 2:
                        for w in late:
                            relay(0, *w)
                    complete(0, s, fresh + peer(s) * part, part)

            return batch(j, False)

        lax.fori_loop(1, heads - 1, middle, 0)
        batch(heads - 1, True)
        return 0

    lax.fori_loop(0, steps, step, 0)
    send_output(steps - 1)

    def finish(g, _):
        for s, t in routes:
            if s != 0 or t != 0:
                query_copy(g, s, t, False).wait_send()
        for d in range(parts):
            output_copy(g, d).wait()
        return 0

    for copy in started:
        copy.wait_send()
    lax.fori_loop(0, steps, finish, 0)


def fused(
    plen, owner, query, fresh_k, fresh_v, cache_k, cache_v, heads, ranks, tps, per_step, chunk
):
    parts = heads * ranks
    few, block = fresh_k.shape[0], cache_k.shape[0]
    fresh = parts * tps * few
    keys = fresh + parts * block
    rows = heads * tps * few
    width = per_step * HEAD_SIZE
    wide = per_step * rows
    own_columns = query.shape[1] // (tps * heads)
    steps = own_columns // width
    rank_sems = []
    count = 4 * heads
    size = ranks
    while size > 1:
        rank_sems += [pltpu.SemaphoreType.DMA((count,))] * 2
        count *= 2
        size //= 2
    dma = pltpu.SemaphoreType.DMA
    b16, f32 = jnp.bfloat16, jnp.float32
    return pl.pallas_call(
        functools.partial(fused_kernel, (heads, ranks, tps, per_step, chunk)),
        out_shape=jax.ShapeDtypeStruct((tps * few, heads * own_columns), b16),
        in_specs=[pl.BlockSpec(memory_space=pltpu.SMEM)] * 2
        + [pl.BlockSpec(memory_space=pl.ANY)] * 5,
        out_specs=pl.BlockSpec(memory_space=pl.ANY),
        scratch_shapes=[
            pltpu.VMEM((keys, 2 * HEAD_SIZE), b16),
            pltpu.VMEM((keys, HEAD_SIZE), b16),
            pltpu.VMEM((HEAD_SIZE, keys), b16),
            pltpu.VMEM((steps, rows, width), b16),
            pltpu.VMEM((rows, own_columns), b16),
            pltpu.VMEM((2 * HEAD_SIZE, wide), b16),
            pltpu.VMEM((rows, rows), b16),
            pltpu.VMEM((per_step, chunk, rows), f32),
            pltpu.VMEM((per_step, chunk, rows), f32),
            pltpu.VMEM((per_step, 1, rows), f32),
            pltpu.VMEM((per_step, 1, rows), f32),
            pltpu.VMEM((per_step, 1, rows), f32),
            pltpu.VMEM((per_step, 1, rows), f32),
            pltpu.VMEM((per_step, HEAD_SIZE, rows), f32),
            dma((2, heads, tps)),
            dma((2, heads, tps)),
            dma((2, heads)),
            dma((2, heads)),
            dma((steps, heads * tps)),
            dma((steps, heads * tps)),
            dma((steps, parts)),
            dma((steps, parts)),
            dma((2 * parts,)),
        ]
        + rank_sems,
        compiler_params=pltpu.CompilerParams(
            collective_id=1, has_side_effects=True, vmem_limit_bytes=56 * 1024 * 1024
        ),
        cost_estimate=pl.CostEstimate(
            flops=4 * rows * own_columns * keys, bytes_accessed=100000000, transcendentals=0
        ),
    )(plen, owner, query, fresh_k, fresh_v, cache_k, cache_v)


def exchanged(
    query,
    fresh_key_rows,
    fresh_value_rows,
    cached_key_rows,
    cached_value_rows,
    prefix_len,
    stripe_owner,
    per_step,
    chunk,
):
    parts, tps = lax.axis_size("cp"), lax.axis_size("tp")
    heads = cached_key_rows.shape[1] // HEAD_SIZE
    ranks = parts // heads
    landed = fused(
        prefix_len,
        stripe_owner,
        query,
        fresh_key_rows,
        fresh_value_rows,
        cached_key_rows,
        cached_value_rows,
        heads,
        ranks,
        tps,
        per_step,
        chunk,
    )
    rows = landed.shape[0]
    stripe = rows // parts
    order = jnp.arange(rows, dtype=jnp.int32).reshape(ranks, heads, stripe)
    order = order.transpose(1, 0, 2).reshape(rows)
    move = (order[:, None] == jnp.arange(rows, dtype=jnp.int32)[None, :]).astype(jnp.bfloat16)
    return jnp.dot(move, landed, preferred_element_type=jnp.float32).astype(jnp.bfloat16)


def plain(
    query, fresh_key_rows, fresh_value_rows, cached_key_rows, cached_value_rows, prefix_len, inverse
):
    parts = lax.axis_size("cp")
    me = lax.axis_index("cp")
    heads = cached_key_rows.shape[1] // HEAD_SIZE
    ranks = parts // heads
    tps = lax.axis_size("tp")
    q_columns = query.shape[1] // tps // heads
    columns = [[h * ranks + r for h in range(heads)] for r in range(ranks)]
    lines = [[h * ranks + r for r in range(ranks)] for h in range(heads)]

    def split_heads(array, axis_name="cp"):
        if heads == 1:
            return array
        return lax.all_to_all(
            array, axis_name, split_axis=1, concat_axis=0, axis_index_groups=columns, tiled=True
        )

    def collect(array):
        block = array.shape[0]
        mine = split_heads(array)
        everything = lax.all_gather(mine, "cp", axis_index_groups=lines, tiled=True)
        return (
            everything.reshape(ranks, heads, block, HEAD_SIZE)
            .transpose(1, 0, 2, 3)
            .reshape(parts * block, HEAD_SIZE)
        )

    q_local = lax.all_to_all(query, "tp", split_axis=1, concat_axis=0, tiled=True)
    rows = q_local.shape[0]
    stripe = rows // parts
    by_rank = inverse.reshape(heads, ranks).T.reshape(-1)
    wanted = (by_rank[:, None] * stripe + jnp.arange(stripe, dtype=jnp.int32)[None, :]).reshape(-1)
    pick = (wanted[:, None] == jnp.arange(rows, dtype=jnp.int32)[None, :]).astype(jnp.bfloat16)
    q_sorted = jnp.dot(pick, q_local, preferred_element_type=jnp.float32).astype(jnp.bfloat16)
    q_out = (
        q_sorted.reshape(ranks, heads * stripe, heads, q_columns)
        .transpose(2, 0, 1, 3)
        .reshape(parts * heads * stripe, q_columns)
    )
    q_mine = lax.all_to_all(q_out, "cp", split_axis=0, concat_axis=0, tiled=True)
    own = [
        lax.all_to_all(array, "tp", split_axis=1, concat_axis=0, tiled=True)
        for array in (fresh_key_rows, fresh_value_rows)
    ]
    cache_k, cache_v, fresh_k, fresh_v = (
        collect(array) for array in (cached_key_rows, cached_value_rows, *own)
    )
    residues = jnp.take(by_rank.reshape(ranks, heads), me % ranks, axis=0)
    nat = (
        jnp.arange(parts, dtype=jnp.int32)[:, None, None] * rows
        + residues[None, :, None] * stripe
        + jnp.arange(stripe, dtype=jnp.int32)[None, None, :]
    ).reshape(1, -1)
    per_step = max(1, min(q_columns // HEAD_SIZE, 512 // nat.shape[1]))
    nat = jnp.tile(nat, (1, per_step))
    done = attend(q_mine, nat, fresh_k, fresh_v, cache_k, cache_v, prefix_len)
    done = (
        done.reshape(parts, heads, stripe, q_columns)
        .transpose(1, 0, 2, 3)
        .reshape(heads * rows, q_columns)
    )
    if heads == 1:
        return done
    split = done.reshape(heads, rows, q_columns)
    back = lax.all_to_all(
        split, "cp", split_axis=0, concat_axis=0, axis_index_groups=columns, tiled=True
    )
    return back.transpose(1, 0, 2).reshape(rows, heads * q_columns)


def shards(
    query,
    fresh_key_rows,
    fresh_value_rows,
    cached_key_rows,
    cached_value_rows,
    prefix_len,
    stripe_owner,
):
    parts, tps = lax.axis_size("cp"), lax.axis_size("tp")
    heads = cached_key_rows.shape[1] // HEAD_SIZE
    ranks = parts // heads
    arrays = (query, fresh_key_rows, fresh_value_rows, cached_key_rows, cached_value_rows)
    rows = heads * tps * fresh_key_rows.shape[0]
    fresh = rows * ranks
    group = query.shape[1] // (tps * heads * HEAD_SIZE)
    per_step, chunk = math.gcd(4, group), 512
    fits = (
        heads > 1
        and heads & (heads - 1) == 0
        and ranks & (ranks - 1) == 0
        and rows % (8 * parts) == 0
        and rows % HEAD_SIZE == 0
        and rows <= 512
        and fresh % (2 * chunk) == 0
        and ranks * cached_key_rows.shape[0] % (2 * chunk) == 0
    )
    if fits:
        return exchanged(*arrays, prefix_len, stripe_owner, per_step, chunk)
    order = jnp.arange(parts, dtype=jnp.int32)
    inverse = jnp.sum(jnp.where(stripe_owner[None, :] == order[:, None], order[None, :], 0), axis=1)
    return plain(*arrays, prefix_len, inverse)


def solution(mesh):
    return jax.shard_map(
        shards,
        mesh=mesh,
        in_specs=(
            P(("cp", "tp"), None),
            P(("cp", "tp"), None),
            P(("cp", "tp"), None),
            P("cp", "tp"),
            P("cp", "tp"),
            P(),
            P(),
        ),
        out_specs=P("cp", "tp"),
        check_vma=False,
    )
```

```python
import functools
import math

import jax
import jax.numpy as jnp
from jax import lax
from jax.experimental import pallas as pl
from jax.experimental.pallas import tpu as pltpu
from jax.sharding import PartitionSpec as P

HEAD_SIZE = 128
NEG = -1e30
EXPONENT = HEAD_SIZE ** (-0.5) * math.log2(math.e)


def attend_kernel(dims, plen_ref, q_ref, nat_ref, fresh_k, fresh_v, cache_k, cache_v, out_ref,
                  k2, vt, q2, s0, s1, m_ref, l_ref, acc_ref):
    per_step, chunk = dims
    rows = q_ref.shape[0]
    wide = rows * per_step
    plen = plen_ref[0]
    fresh, slots = fresh_k.shape[0], cache_k.shape[0]
    dn = (((1,), (1,)), ((), ()))

    @pl.when(pl.program_id(0) == 0)
    def _():
        eye = (lax.broadcasted_iota(jnp.int32, (HEAD_SIZE, HEAD_SIZE), 0)
               == lax.broadcasted_iota(jnp.int32, (HEAD_SIZE, HEAD_SIZE), 1)).astype(jnp.bfloat16)
        step = min(512, fresh)

        def prepare(source_k, source_v, base, count):
            def body(b, _):
                at = pl.multiple_of(b * step, step)
                to = pl.multiple_of(base + b * step, step)
                k = source_k[pl.ds(at, step), :]
                k2[pl.ds(to, step), :HEAD_SIZE] = k
                k2[pl.ds(to, step), HEAD_SIZE:] = k
                v = source_v[pl.ds(at, step), :]
                vt[:, pl.ds(to, step)] = lax.dot_general(
                    eye, v, dn, preferred_element_type=jnp.float32).astype(jnp.bfloat16)
                return 0
            lax.fori_loop(0, count // step, body, 0)
        prepare(fresh_k, fresh_v, 0, fresh)
        prepare(cache_k, cache_v, fresh, slots)

    for g in range(per_step):
        x = q_ref[:, g * HEAD_SIZE:(g + 1) * HEAD_SIZE].astype(jnp.float32) * EXPONENT
        x = x.T
        hi = x.astype(jnp.bfloat16)
        q2[:HEAD_SIZE, g * rows:(g + 1) * rows] = hi
        q2[HEAD_SIZE:, g * rows:(g + 1) * rows] = (x - hi.astype(jnp.float32)).astype(jnp.bfloat16)

    def score(at, s):
        s[...] = jnp.dot(k2[pl.ds(at, chunk), :], q2[...], preferred_element_type=jnp.float32)

    def soften(at, s_ref, mask, first):
        s = s_ref[...]
        if mask is not None:
            s = jnp.where(mask, s, NEG)
        top = jnp.max(s, axis=0, keepdims=True)
        m_new = top if first else jnp.maximum(m_ref[...], top)
        p = jnp.exp2(s - m_new)
        total = jnp.sum(p, axis=0, keepdims=True)
        o = jnp.dot(vt[:, pl.ds(at, chunk)], p.astype(jnp.bfloat16), preferred_element_type=jnp.float32)
        if first:
            l_ref[...] = total
            acc_ref[...] = o
        else:
            f = jnp.exp2(m_ref[...] - m_new)
            l_ref[...] = f * l_ref[...] + total
            acc_ref[...] = f * acc_ref[...] + o
        m_ref[...] = m_new

    bufs = (s0, s1)
    number = fresh // chunk
    assert number % 2 == 0
    nat = nat_ref[...]
    index = lax.broadcasted_iota(jnp.int32, (chunk, wide), 0)
    score(0, s0)
    for c in range(number):
        score((c + 1) * chunk, bufs[(c + 1) % 2])
        soften(c * chunk, bufs[c % 2], index + c * chunk <= nat, c == 0)

    pairs = (plen + 2 * chunk - 1) // (2 * chunk)

    def body(j, _):
        at = pl.multiple_of(fresh + 2 * j * chunk, chunk)
        score(pl.multiple_of(at + chunk, chunk), s1)
        soften(at, s0, None, False)
        score(pl.multiple_of(at + 2 * chunk, chunk), s0)
        soften(pl.multiple_of(at + chunk, chunk), s1, None, False)
        return 0
    lax.fori_loop(0, pairs - 1, body, 0)
    slot = 2 * (pairs - 1) * chunk
    at = pl.multiple_of(fresh + slot, chunk)
    score(pl.multiple_of(at + chunk, chunk), s1)
    soften(at, s0, index + slot < plen, False)
    soften(pl.multiple_of(at + chunk, chunk), s1, index + (slot + chunk) < plen, False)

    done = acc_ref[...] / l_ref[...]
    for g in range(per_step):
        out_ref[:, g * HEAD_SIZE:(g + 1) * HEAD_SIZE] = done[:, g * rows:(g + 1) * rows].T.astype(out_ref.dtype)


def attend(q, nat, fresh_k, fresh_v, cache_k, cache_v, prefix_len, chunk=512):
    rows, columns = q.shape
    per_step = nat.shape[1] // rows
    width = per_step * HEAD_SIZE
    wide = per_step * rows
    fresh, slots = fresh_k.shape[0], cache_k.shape[0]
    whole = lambda i, *_: (0, 0)
    keys = fresh + slots
    return pl.pallas_call(
        functools.partial(attend_kernel, (per_step, chunk)),
        out_shape=jax.ShapeDtypeStruct((rows, columns), jnp.bfloat16),
        grid_spec=pltpu.PrefetchScalarGridSpec(
            num_scalar_prefetch=1,
            grid=(columns // width,),
            in_specs=[
                pl.BlockSpec((rows, width), lambda i, *_: (0, i)),
                pl.BlockSpec((1, wide), whole),
                pl.BlockSpec((fresh, HEAD_SIZE), whole),
                pl.BlockSpec((fresh, HEAD_SIZE), whole),
                pl.BlockSpec((slots, HEAD_SIZE), whole),
                pl.BlockSpec((slots, HEAD_SIZE), whole),
            ],
            out_specs=pl.BlockSpec((rows, width), lambda i, *_: (0, i)),
            scratch_shapes=[
                pltpu.VMEM((keys, 2 * HEAD_SIZE), jnp.bfloat16),
                pltpu.VMEM((HEAD_SIZE, keys), jnp.bfloat16),
                pltpu.VMEM((2 * HEAD_SIZE, wide), jnp.bfloat16),
                pltpu.VMEM((chunk, wide), jnp.float32),
                pltpu.VMEM((chunk, wide), jnp.float32),
                pltpu.VMEM((1, wide), jnp.float32),
                pltpu.VMEM((1, wide), jnp.float32),
                pltpu.VMEM((HEAD_SIZE, wide), jnp.float32),
            ],
        ),
        compiler_params=pltpu.CompilerParams(vmem_limit_bytes=56 * 1024 * 1024),
        cost_estimate=pl.CostEstimate(flops=4*rows*columns*keys, bytes_accessed=4 * keys*HEAD_SIZE, transcendentals=0),
    )(prefix_len, q, nat, fresh_k, fresh_v, cache_k, cache_v)


def remote(source, target, send, receive, device):
    return pltpu.make_async_remote_copy(
        src_ref=source,
        dst_ref=target,
        send_sem=send,
        recv_sem=receive,
        device_id=device,
        device_id_type=pl.DeviceIdType.MESH,
    )


def greet(devices):
    barrier = pltpu.get_barrier_semaphore()
    for device in devices:
        pl.semaphore_signal(
            barrier, inc=1, device_id=device, device_id_type=pl.DeviceIdType.MESH
        )
    pl.semaphore_wait(barrier, len(devices))


def fused_kernel(
    sizes,
    plen_ref,
    owner_ref,
    query,
    fresh_k,
    fresh_v,
    cache_k,
    cache_v,
    out,
    k2,
    v_land,
    vt,
    q_land,
    o_buf,
    q2,
    pick_ref,
    s0,
    s1,
    t0,
    t1,
    m_ref,
    l_ref,
    acc_ref,
    fresh_send,
    fresh_recv,
    z_send,
    z_recv,
    q_send,
    q_recv,
    o_send,
    o_recv,
    twin_sem,
    *rank_sems,
):
    heads, ranks, tps, per_step, chunk = sizes
    parts = heads * ranks
    me, tp = lax.axis_index("cp"), lax.axis_index("tp")
    row, rank = me // ranks, me % ranks
    few = fresh_k.shape[0]
    block = cache_k.shape[0]
    fresh = parts * tps * few
    keys = k2.shape[0]
    slots = keys - fresh
    steps, rows, width = q_land.shape
    own_columns = steps * width
    wide = per_step * rows
    share = rows // parts
    dn = (((1,), (1,)), ((), ()))

    bits = []
    bit = ranks // 2
    while bit:
        bits.append(bit)
        bit //= 2
    partners = [rank + bit - 2 * bit * ((rank // bit) % 2) for bit in bits]
    line = [{"cp": row * ranks + partner} for partner in partners]

    def peer(s):
        other = row
        bit = 1
        while bit < heads:
            other = other + (s // bit) % 2 * (bit - 2 * bit * ((other // bit) % 2))
            bit *= 2
        return other

    def at_column(s, t):
        return {"cp": peer(s) * ranks + rank, "tp": (tp + t) % tps}

    greet(
        [{"cp": (me + d) % parts} for d in range(1, parts)]
        + [at_column(s, t) for s in range(heads) for t in range(1, tps)]
    )

    def span(ref, start, size, step):
        return ref.at[pl.ds(pl.multiple_of(start, step), size), pl.ds(0, HEAD_SIZE)]

    def cut(ref, head):
        return ref.at[:, pl.ds(pl.multiple_of(head * HEAD_SIZE, HEAD_SIZE), HEAD_SIZE)]

    def place(a, index):
        target = k2 if a % 2 == 0 else v_land
        if a < 2:
            return span(target, fresh + index * block, block, block)
        return span(target, index * (tps * few), tps * few, tps * few)

    shifts = range(heads)
    started = []

    def go(copy):
        copy.start()
        started.append(copy)
        return copy

    arrived = {}
    for s in shifts:
        for a, source in enumerate((fresh_k, fresh_v)):
            waits = []
            for t in range(tps):
                to = at_column(s, t)
                piece = cut(source, to["tp"] * heads + peer(s))
                target = span((k2, v_land)[a], me * (tps * few) + tp * few, few, few)
                if s == 0 and t == 0:
                    copy = pltpu.make_async_copy(piece, target, fresh_recv.at[a, s, t])
                    copy.start()
                    waits.append(copy.wait)
                else:
                    copy = go(
                        remote(
                            piece, target, fresh_send.at[a, s, t], fresh_recv.at[a, s, t], to
                        )
                    )
                    waits.append(copy.wait_recv)
            arrived[2 + a, s, 0] = waits
    for s in shifts:
        for a, source in enumerate((cache_k, cache_v)):
            piece = cut(source, peer(s))
            if s == 0:
                copy = pltpu.make_async_copy(piece, place(a, me), z_recv.at[a, s])
                copy.start()
                arrived[a, s, 0] = [copy.wait]
            else:
                copy = go(
                    remote(piece, place(a, me), z_send.at[a, s], z_recv.at[a, s], at_column(s, 0))
                )
                arrived[a, s, 0] = [copy.wait_recv]

    def query_copy(g, s, t, local):
        to = at_column(s, t)
        start = (to["tp"] * heads + peer(s)) * own_columns + g * width
        source = query.at[:, pl.ds(pl.multiple_of(start, width), width)]
        target = q_land.at[g, pl.ds(pl.multiple_of((row * tps + tp) * few, few), few), :]
        if local:
            return pltpu.make_async_copy(source, target, q_recv.at[g, 0])
        return remote(source, target, q_send.at[g, s * tps + t], q_recv.at[g, s * tps + t], to)

    routes = [(s, t) for s in shifts for t in range(tps)]

    def send_query(g, _):
        for s, t in routes:
            query_copy(g, s, t, s == 0 and t == 0).start()
        return 0

    lax.fori_loop(0, steps, send_query, 0)

    relays, held = {}, {}
    for s in shifts:
        for a in range(4):
            mine = [((a, s, 0), rank)]
            for level, partner in enumerate(partners):
                send, receive = rank_sems[2 * level], rank_sems[2 * level + 1]
                bit = bits[level]
                other = []
                for k, (key, owner) in enumerate(mine):
                    number = (s * 4 + a) * 2**level + k
                    piece = place(a, peer(s) * ranks + owner)
                    copy = remote(piece, piece, send.at[number], receive.at[number], line[level])
                    started.append(copy)
                    relays.setdefault((a // 2, s, level), []).append((key, copy))
                    name = (a, s, level + 1, k)
                    arrived[name] = [copy.wait_recv]
                    other.append((name, owner + bit - 2 * bit * ((owner // bit) % 2)))
                mine = mine + other
            for key, owner in mine:
                index = peer(s) * ranks + owner
                held.setdefault((a // 2, s), []).append((key, a, index))
    twin_copies = {}
    for kind, s in held:
        for key, a, index in held[kind, s]:
            if a % 2 == 0:
                size = tps * few if kind else block
                start = index * size + (0 if kind else fresh)
                twin_copies[key] = pltpu.make_async_copy(
                    span(k2, start, size, size),
                    k2.at[pl.ds(pl.multiple_of(start, size), size), pl.ds(HEAD_SIZE, HEAD_SIZE)],
                    twin_sem.at[len(twin_copies)],
                )

    def relay(kind, s, level):
        for key, copy in relays[kind, s, level]:
            if key[2] == level:
                for wait in arrived[key]:
                    wait()
            copy.start()

    levels = len(partners)
    waves = sorted(((s, l) for s in shifts for l in range(levels)), key=lambda w: (sum(w), w[1]))
    early = [w for w in waves if sum(w) < heads or heads <= 2]
    late = [w for w in waves if w not in early]
    for number, (s, level) in enumerate(early):
        relay(0, s, level)
        if s == 0:
            for other in shifts:
                relay(1, other, level)

    lane = lax.broadcasted_iota(jnp.int32, (rows, rows), 1)
    sorted_row = lax.broadcasted_iota(jnp.int32, (rows, rows), 0)

    def natural(at):
        many = tps * few
        stripe = many // parts
        inside = jnp.zeros(at.shape, jnp.int32)
        for r in range(parts):
            inside = jnp.where(at // share == owner_ref[r], r * stripe, inside)
        return at % share // stripe, inside + at % stripe

    z, inside = natural(sorted_row)
    pick_ref[...] = (z * (tps * few) + inside == lane).astype(jnp.float32).astype(jnp.bfloat16)

    eye = (
        lax.broadcasted_iota(jnp.int32, (HEAD_SIZE, HEAD_SIZE), 0)
        == lax.broadcasted_iota(jnp.int32, (HEAD_SIZE, HEAD_SIZE), 1)
    ).astype(jnp.bfloat16)

    def complete(kind, s, base, count):
        items = held[kind, s]
        for key, a, index in items:
            if key[2] == levels:
                for wait in arrived[key]:
                    wait()
            if key in twin_copies:
                twin_copies[key].start()

        def prepare(b, _):
            at = pl.multiple_of(base + b * chunk, chunk)
            vt[:, pl.ds(at, chunk)] = lax.dot_general(
                eye, v_land[pl.ds(at, chunk), :], dn, preferred_element_type=jnp.float32
            ).astype(jnp.bfloat16)
            return 0

        lax.fori_loop(0, count // chunk, prepare, 0)
        for key, a, index in items:
            if key in twin_copies:
                twin_copies[key].wait()

    for s in shifts:
        complete(1, s, 0, fresh if s == heads - 1 else 0)
    part = ranks * block
    for s in range(2):
        complete(0, s, fresh + peer(s) * part, part)

    slabs = ((s0, t0), (s1, t1))

    def score(at, slab, h, mask):
        s_ref, t_ref = slabs[slab]
        s = jnp.dot(
            k2[pl.ds(at, chunk), :],
            q2[:, h * rows : (h + 1) * rows],
            preferred_element_type=jnp.float32,
        )
        if mask is not None:
            s = jnp.where(mask, s, NEG)
        s_ref[h] = s
        t_ref[h] = jnp.max(s, axis=0, keepdims=True)

    def soften(at, slab, h, first):
        s_ref, t_ref = slabs[slab]
        top = t_ref[h]
        m_new = top if first else jnp.maximum(m_ref[h], top)
        p = jnp.exp2(s_ref[h] - m_new)
        total = jnp.sum(p, axis=0, keepdims=True)
        o = jnp.dot(
            vt[:, pl.ds(at, chunk)], p.astype(jnp.bfloat16), preferred_element_type=jnp.float32
        )
        if first:
            l_ref[h] = total
            acc_ref[h] = o
        else:
            f = jnp.exp2(m_ref[h] - m_new)
            l_ref[h] = f * l_ref[h] + total
            acc_ref[h] = f * acc_ref[h] + o
        m_ref[h] = m_new

    def output_copy(g, d):
        to = peer(d // ranks) * ranks + (rank + d % ranks) % ranks
        columns = pl.ds(pl.multiple_of(g * width, width), width)
        source = o_buf.at[pl.ds(pl.multiple_of(to * share, share), share), columns]
        target = out.at[
            pl.ds(pl.multiple_of(rank * share, share), share),
            pl.ds(pl.multiple_of(row * own_columns + g * width, width), width),
        ]
        if d == 0:
            return pltpu.make_async_copy(source, target, o_recv.at[g, 0])
        return remote(source, target, o_send.at[g, d], o_recv.at[g, d], {"cp": to})

    def send_output(g):
        for d in range(parts):
            output_copy(g, d).start()

    number = fresh // chunk
    units = slots // chunk
    group = part // chunk
    index = lax.broadcasted_iota(jnp.int32, (chunk, rows), 0)

    def step(g, _):
        for s, t in routes:
            if s == 0 and t == 0:
                query_copy(g, s, t, True).wait()
            else:
                query_copy(g, s, t, False).wait_recv()
        for h in range(per_step):
            x = jnp.dot(
                pick_ref[...],
                q_land[g, :, h * HEAD_SIZE : (h + 1) * HEAD_SIZE],
                preferred_element_type=jnp.float32,
            )
            x = x.T * EXPONENT
            hi = x.astype(jnp.bfloat16)
            q2[:HEAD_SIZE, h * rows : (h + 1) * rows] = hi
            q2[HEAD_SIZE:, h * rows : (h + 1) * rows] = (x - hi.astype(jnp.float32)).astype(
                jnp.bfloat16
            )

        @pl.when(g > 0)
        def _():
            send_output(g - 1)

        def base_of(s):
            return pl.multiple_of(fresh + peer(s) * part, chunk)

        z, inside = natural(lax.broadcasted_iota(jnp.int32, (1, rows), 1))
        nat = (z * ranks + rank) * (tps * few) + inside
        for h in range(per_step):
            score(0, 0, h, index <= nat)
        for c in range(number):
            for h in range(per_step):
                if c + 1 < number:
                    score((c + 1) * chunk, (c + 1) % 2, h, index + (c + 1) * chunk <= nat)
                else:
                    score(base_of(0), 0, h, index + peer(0) * part < plen_ref[0])
                soften(c * chunk, c % 2, h, c == 0)

        def batch(j, last):
            here = peer(j) * part
            beyond = None if last else peer(j + 1) * part
            for u in range(group):
                slot = here + u * chunk
                after = slot + chunk if u + 1 < group else beyond
                for h in range(per_step):
                    if after is not None:
                        score(
                            pl.multiple_of(fresh + after, chunk),
                            (u + 1) % 2,
                            h,
                            index + after < plen_ref[0],
                        )
                    soften(pl.multiple_of(fresh + slot, chunk), u % 2, h, False)
                    if after is None:
                        finish_head(h)
            return 0

        def finish_head(h):
            columns = pl.ds(pl.multiple_of(g * width + h * HEAD_SIZE, HEAD_SIZE), HEAD_SIZE)
            o_buf[:, columns] = (acc_ref[h] / l_ref[h]).T.astype(o_buf.dtype)

        batch(0, False)

        def middle(j, _):
            for s in range(2, heads):

                @pl.when((g == 0) & (j == s - 1))
                def _():
                    if s == 2:
                        for w in late:
                            relay(0, *w)
                    complete(0, s, fresh + peer(s) * part, part)

            return batch(j, False)

        lax.fori_loop(1, heads - 1, middle, 0)
        batch(heads - 1, True)
        return 0

    lax.fori_loop(0, steps, step, 0)
    send_output(steps - 1)

    def finish(g, _):
        for s, t in routes:
            if s != 0 or t != 0:
                query_copy(g, s, t, False).wait_send()
        for d in range(parts):
            output_copy(g, d).wait()
        return 0

    for copy in started:
        copy.wait_send()
    lax.fori_loop(0, steps, finish, 0)


def fused(
    plen, owner, query, fresh_k, fresh_v, cache_k, cache_v, heads, ranks, tps, per_step, chunk
):
    parts = heads * ranks
    few, block = fresh_k.shape[0], cache_k.shape[0]
    fresh = parts * tps * few
    keys = fresh + parts * block
    rows = heads * tps * few
    width = per_step * HEAD_SIZE
    wide = per_step * rows
    own_columns = query.shape[1] // (tps * heads)
    steps = own_columns // width
    rank_sems = []
    count = 4 * heads
    size = ranks
    while size > 1:
        rank_sems += [pltpu.SemaphoreType.DMA((count,))] * 2
        count *= 2
        size //= 2
    dma = pltpu.SemaphoreType.DMA
    b16, f32 = jnp.bfloat16, jnp.float32
    return pl.pallas_call(
        functools.partial(fused_kernel, (heads, ranks, tps, per_step, chunk)),
        out_shape=jax.ShapeDtypeStruct((tps * few, heads * own_columns), b16),
        in_specs=[pl.BlockSpec(memory_space=pltpu.SMEM)] * 2
        + [pl.BlockSpec(memory_space=pl.ANY)] * 5,
        out_specs=pl.BlockSpec(memory_space=pl.ANY),
        scratch_shapes=[
            pltpu.VMEM((keys, 2 * HEAD_SIZE), b16),
            pltpu.VMEM((keys, HEAD_SIZE), b16),
            pltpu.VMEM((HEAD_SIZE, keys), b16),
            pltpu.VMEM((steps, rows, width), b16),
            pltpu.VMEM((rows, own_columns), b16),
            pltpu.VMEM((2 * HEAD_SIZE, wide), b16),
            pltpu.VMEM((rows, rows), b16),
            pltpu.VMEM((per_step, chunk, rows), f32),
            pltpu.VMEM((per_step, chunk, rows), f32),
            pltpu.VMEM((per_step, 1, rows), f32),
            pltpu.VMEM((per_step, 1, rows), f32),
            pltpu.VMEM((per_step, 1, rows), f32),
            pltpu.VMEM((per_step, 1, rows), f32),
            pltpu.VMEM((per_step, HEAD_SIZE, rows), f32),
            dma((2, heads, tps)),
            dma((2, heads, tps)),
            dma((2, heads)),
            dma((2, heads)),
            dma((steps, heads * tps)),
            dma((steps, heads * tps)),
            dma((steps, parts)),
            dma((steps, parts)),
            dma((2 * parts,)),
        ]
        + rank_sems,
        compiler_params=pltpu.CompilerParams(
            collective_id=1, has_side_effects=True, vmem_limit_bytes=56 * 1024 * 1024
        ),
        cost_estimate=pl.CostEstimate(
            flops=4 * rows * own_columns * keys, bytes_accessed=100000000, transcendentals=0
        ),
    )(plen, owner, query, fresh_k, fresh_v, cache_k, cache_v)


def exchanged(
    query,
    fresh_key_rows,
    fresh_value_rows,
    cached_key_rows,
    cached_value_rows,
    prefix_len,
    stripe_owner,
    per_step,
    chunk,
):
    parts, tps = lax.axis_size("cp"), lax.axis_size("tp")
    heads = cached_key_rows.shape[1] // HEAD_SIZE
    ranks = parts // heads
    landed = fused(
        prefix_len,
        stripe_owner,
        query,
        fresh_key_rows,
        fresh_value_rows,
        cached_key_rows,
        cached_value_rows,
        heads,
        ranks,
        tps,
        per_step,
        chunk,
    )
    rows = landed.shape[0]
    stripe = rows // parts
    order = jnp.arange(rows, dtype=jnp.int32).reshape(ranks, heads, stripe)
    order = order.transpose(1, 0, 2).reshape(rows)
    move = (order[:, None] == jnp.arange(rows, dtype=jnp.int32)[None, :]).astype(jnp.bfloat16)
    return jnp.dot(move, landed, preferred_element_type=jnp.float32).astype(jnp.bfloat16)


def plain(
    query, fresh_key_rows, fresh_value_rows, cached_key_rows, cached_value_rows, prefix_len, inverse
):
    parts = lax.axis_size("cp")
    me = lax.axis_index("cp")
    heads = cached_key_rows.shape[1] // HEAD_SIZE
    ranks = parts // heads
    tps = lax.axis_size("tp")
    q_columns = query.shape[1] // tps // heads
    columns = [[h * ranks + r for h in range(heads)] for r in range(ranks)]
    lines = [[h * ranks + r for r in range(ranks)] for h in range(heads)]

    def split_heads(array, axis_name="cp"):
        if heads == 1:
            return array
        return lax.all_to_all(
            array, axis_name, split_axis=1, concat_axis=0, axis_index_groups=columns, tiled=True
        )

    def collect(array):
        block = array.shape[0]
        mine = split_heads(array)
        everything = lax.all_gather(mine, "cp", axis_index_groups=lines, tiled=True)
        return (
            everything.reshape(ranks, heads, block, HEAD_SIZE)
            .transpose(1, 0, 2, 3)
            .reshape(parts * block, HEAD_SIZE)
        )

    q_local = lax.all_to_all(query, "tp", split_axis=1, concat_axis=0, tiled=True)
    rows = q_local.shape[0]
    stripe = rows // parts
    by_rank = inverse.reshape(heads, ranks).T.reshape(-1)
    wanted = (by_rank[:, None] * stripe + jnp.arange(stripe, dtype=jnp.int32)[None, :]).reshape(-1)
    pick = (wanted[:, None] == jnp.arange(rows, dtype=jnp.int32)[None, :]).astype(jnp.bfloat16)
    q_sorted = jnp.dot(pick, q_local, preferred_element_type=jnp.float32).astype(jnp.bfloat16)
    q_out = (
        q_sorted.reshape(ranks, heads * stripe, heads, q_columns)
        .transpose(2, 0, 1, 3)
        .reshape(parts * heads * stripe, q_columns)
    )
    q_mine = lax.all_to_all(q_out, "cp", split_axis=0, concat_axis=0, tiled=True)
    own = [
        lax.all_to_all(array, "tp", split_axis=1, concat_axis=0, tiled=True)
        for array in (fresh_key_rows, fresh_value_rows)
    ]
    cache_k, cache_v, fresh_k, fresh_v = (
        collect(array) for array in (cached_key_rows, cached_value_rows, *own)
    )
    residues = jnp.take(by_rank.reshape(ranks, heads), me % ranks, axis=0)
    nat = (
        jnp.arange(parts, dtype=jnp.int32)[:, None, None] * rows
        + residues[None, :, None] * stripe
        + jnp.arange(stripe, dtype=jnp.int32)[None, None, :]
    ).reshape(1, -1)
    per_step = max(1, min(q_columns // HEAD_SIZE, 512 // nat.shape[1]))
    nat = jnp.tile(nat, (1, per_step))
    done = attend(q_mine, nat, fresh_k, fresh_v, cache_k, cache_v, prefix_len)
    done = (
        done.reshape(parts, heads, stripe, q_columns)
        .transpose(1, 0, 2, 3)
        .reshape(heads * rows, q_columns)
    )
    if heads == 1:
        return done
    split = done.reshape(heads, rows, q_columns)
    back = lax.all_to_all(
        split, "cp", split_axis=0, concat_axis=0, axis_index_groups=columns, tiled=True
    )
    return back.transpose(1, 0, 2).reshape(rows, heads * q_columns)


def shards(
    query,
    fresh_key_rows,
    fresh_value_rows,
    cached_key_rows,
    cached_value_rows,
    prefix_len,
    stripe_owner,
):
    parts, tps = lax.axis_size("cp"), lax.axis_size("tp")
    heads = cached_key_rows.shape[1] // HEAD_SIZE
    ranks = parts // heads
    arrays = (query, fresh_key_rows, fresh_value_rows, cached_key_rows, cached_value_rows)
    rows = heads * tps * fresh_key_rows.shape[0]
    fresh = rows * ranks
    group = query.shape[1] // (tps * heads * HEAD_SIZE)
    per_step, chunk = math.gcd(4, group), 512
    fits = (
        heads > 1
        and heads & (heads - 1) == 0
        and ranks & (ranks - 1) == 0
        and rows % (8 * parts) == 0
        and rows % HEAD_SIZE == 0
        and rows <= 512
        and fresh % (2 * chunk) == 0
        and ranks * cached_key_rows.shape[0] % (2 * chunk) == 0
    )
    if fits:
        return exchanged(*arrays, prefix_len, stripe_owner, per_step, chunk)
    order = jnp.arange(parts, dtype=jnp.int32)
    inverse = jnp.sum(jnp.where(stripe_owner[None, :] == order[:, None], order[None, :], 0), axis=1)
    return plain(*arrays, prefix_len, inverse)


def solution(mesh):
    return jax.shard_map(
        shards,
        mesh=mesh,
        in_specs=(
            P(("cp", "tp"), None),
            P(("cp", "tp"), None),
            P(("cp", "tp"), None),
            P("cp", "tp"),
            P("cp", "tp"),
            P(),
            P(),
        ),
        out_specs=P("cp", "tp"),
        check_vma=False,
    )
```
